32 devices in a mesh: pts: 16 (over z, y, core), cen: 2 (over x).
Axes of the slice: x: 2, y: 2, z: 4, core: 2. Of those that a mesh axis runs over, the one named last changes fastest.
Arguments:
- points: bfloat16 [4096, 256], P('pts'), may hold values from -64 to 64
- centroids: bfloat16 [65536, 256], P('cen'), may hold values from -10 to 10
Outputs:
- updated: float32 [65536, 256], P(('cen', 'pts'))
- log_norm: float32 [4096], P('pts')
The draws below stay inside these ranges and needn't reach their ends.
All inputs are finite; a program needn't handle non-finite values.
Results may differ from the reference program's by a relative error of at most 0.0017.
Values may be sent and summed in bfloat16 or wider, within the bound.
A program may use at most 128 MiB of HBM per device.

```python
import math
import jax
import jax.numpy as jnp
from jax import lax

D = 256
K = 65536
NPTS = 4096


def centroid_table(key):
    table = jnp.clip(jax.random.normal(jax.random.fold_in(key, 11), (K, D), jnp.float32), -6.0, 6.0)
    return table


def draw_centroids(key, part):
    return centroid_table(key).astype(jnp.bfloat16)


def draw_points(key, part):
    values = jnp.clip(jax.random.normal(jax.random.fold_in(key, 21), (NPTS, D), jnp.float32), -6.0, 6.0)
    return values.astype(jnp.bfloat16)


def setup_inputs(seed: int = 0) -> dict:
    keys = jax.random.split(jax.random.key(seed), 3)
    return {
        "points": draw_points(jax.random.fold_in(keys[2], 71), 0),
        "centroids": draw_centroids(jax.random.fold_in(keys[2], 71), 0),
    }


inv_temp = 0.0625
prior_count = 1.0


def reference(points, centroids):
    center_norms = jnp.sum(jnp.square(centroids.astype(jnp.float32)), axis=1)
    block_rows = math.gcd(NPTS, 1024)
    batches = points.reshape(NPTS // block_rows, block_rows, D)

    def one_block(totals, batch_rows):
        weighted, masses = totals
        logits = (2.0 * lax.dot_general(batch_rows, centroids, (((1,), (1,)), ((), ())), preferred_element_type=jnp.float32) - center_norms[None, :]) * inv_temp
        peak = jnp.max(logits, axis=1)
        row_log = peak + jnp.log(jnp.sum(jnp.exp(logits - peak[:, None]), axis=1))
        shares = jnp.exp(logits - row_log[:, None]).astype(jnp.bfloat16)
        weighted = weighted + lax.dot_general(shares, batch_rows, (((0,), (0,)), ((), ())), preferred_element_type=jnp.float32)
        masses = masses + jnp.sum(shares.astype(jnp.float32), axis=0)
        return (weighted, masses), row_log

    start = (jnp.zeros((K, D), jnp.float32), jnp.zeros((K,), jnp.float32))
    (weighted, masses), row_logs = lax.scan(one_block, start, batches)
    updated = (centroids.astype(jnp.float32) + weighted) / (prior_count + masses)[:, None]
    return updated, row_logs.reshape(NPTS)
```

```python
import functools
import math

import jax
import jax.numpy as jnp
from jax import lax
from jax.experimental import pallas as pl
from jax.experimental.pallas import tpu as pltpu
from jax.sharding import PartitionSpec as P

inv_temp = 0.0625
prior_count = 1.0
log2e = math.log2(math.e)
MESH = pl.DeviceIdType.MESH


def kernel(
    G, C, points_ref, table_ref, out_ref, norm_ref,
    pts_all, pts_scaled, table, half_norms, scores, shares,
    peaks, local_log, all_local, every_norm, factors,
    load_sem, send_sem, ring_sem, twin_sem, stat_send, stat_recv, norm_send, norm_recv,
):
    T, D = points_ref.shape
    own = table.shape[0]
    R = G // 2
    far = R // 2
    half = T // 2
    W = T // 128
    N = G * C
    RB = min(256, own)
    NB = own // RB
    me = lax.axis_index("pts")
    cen = lax.axis_index("cen")
    mine = cen * G + me
    core = me % 2
    chip = me // 2
    turn = chip % 2
    pos = (chip // 2) * (1 - turn) + (R - 1 - chip // 2) * turn

    def tile_at(p, c):
        s = p // far
        return ((1 - s) * 2 * p + s * (2 * (R - 1 - p) + 1)) * 2 + c

    twin = me + 1 - 2 * core
    right = tile_at((pos + 1) % R, core)
    left = tile_at((pos + R - 1) % R, core)

    my_points = pts_all.at[pl.ds(pl.multiple_of(me * T, T), T)]
    load_points = pltpu.make_async_copy(points_ref, my_points, load_sem.at[0])
    load_points.start()
    load_table = pltpu.make_async_copy(
        table_ref.at[pl.ds(pl.multiple_of(me * own, own), own)], table, load_sem.at[1]
    )
    load_table.start()

    barrier = pltpu.get_barrier_semaphore()

    for peer in (right, left, twin):
        pl.semaphore_signal(
            barrier, inc=1, device_id={"pts": peer, "cen": cen}, device_id_type=MESH
        )
    for i in range(1, C):
        pl.semaphore_signal(
            barrier, inc=1, device_id={"pts": me, "cen": (cen + i) % C}, device_id_type=MESH
        )
    load_points.wait()
    pl.semaphore_wait(barrier, 2 + C)

    def rows_of(t, h):
        return pts_all.at[pl.ds(pl.multiple_of(t * T + h * half, half), half)]

    def from_left(d):
        return tile_at((pos + R - d) % R, core)

    def from_right(d):
        return tile_at((pos + d) % R, core)

    def ring_copy(way, d, h, t):
        return pltpu.make_async_remote_copy(
            src_ref=rows_of(t, h), dst_ref=rows_of(t, h), send_sem=send_sem,
            recv_sem=ring_sem.at[way, d, h],
            device_id={"pts": (right, left)[way], "cen": cen}, device_id_type=MESH,
        )

    def twin_copy(way, d, h, t):
        return pltpu.make_async_remote_copy(
            src_ref=rows_of(t, h), dst_ref=rows_of(t, h), send_sem=send_sem,
            recv_sem=twin_sem.at[way, d, h],
            device_id={"pts": twin, "cen": cen}, device_id_type=MESH,
        )

    for h in range(2):
        ring_copy(0, 1, h, me).start()
        ring_copy(1, 1, 1 - h, me).start()
    for h in range(2):
        twin_copy(0, 0, h, me).start()

    load_table.wait()

    def norms(r, carry):
        rows = pl.ds(pl.multiple_of(r * RB, RB), RB)
        block = table[rows, :].astype(jnp.float32)
        total = jnp.sum(block * block, axis=1, keepdims=True)
        half_norms[rows, :] = jnp.broadcast_to(0.5 * total, (RB, T))
        return carry

    lax.fori_loop(0, NB, norms, 0)

    def process(t):
        cols = pl.ds(pl.multiple_of(t * T, T), T)
        tile = pts_all[cols, :]

        def score(r, top):
            rows = pl.ds(pl.multiple_of(r * RB, RB), RB)
            u = lax.dot_general(
                table[rows, :], tile, (((1,), (1,)), ((), ())),
                preferred_element_type=jnp.float32,
            ) - half_norms[rows, :]
            scores[rows, :] = u
            return jnp.maximum(top, jnp.max(u.reshape(RB // 8, 8, T), axis=0))

        top = lax.fori_loop(
            0, NB, score, jnp.full((8, T), -jnp.inf, jnp.float32), unroll=True
        )
        peak = jnp.max(top, axis=0, keepdims=True)

        def weigh(r, total):
            rows = pl.ds(pl.multiple_of(r * RB, RB), RB)
            e = jnp.exp2((scores[rows, :] - peak) * (2.0 * inv_temp * log2e))
            packed = e.astype(jnp.bfloat16)
            for g in range(W):
                shares[t * W + g, rows, :] = packed[:, g * 128:(g + 1) * 128]
            return total + jnp.sum(e.reshape(RB // 8, 8, T), axis=0)

        total = lax.fori_loop(0, NB, weigh, jnp.zeros((8, T), jnp.float32), unroll=True)
        scaled_peak = peak * (2.0 * inv_temp)
        peaks[t] = scaled_peak
        value = scaled_peak + jnp.log(jnp.sum(total, axis=0, keepdims=True))
        local_log[t] = value

        @pl.when(t == me)
        def _():
            all_local[mine] = value

        def tell(c, carry):
            @pl.when(c * G + t != mine)
            def _():
                pltpu.make_async_remote_copy(
                    src_ref=local_log.at[t], dst_ref=all_local.at[mine],
                    send_sem=stat_send, recv_sem=stat_recv,
                    device_id={"pts": t, "cen": c}, device_id_type=MESH,
                ).start()
            return carry

        lax.fori_loop(0, C, tell, 0)

    other = 1 - 2 * core

    def twin_ready(way, d, t):
        for h in range(2):
            twin_copy(way, d, h, t).wait_recv()

    process(me)

    def step(d, carry):
        a, b = from_left(d), from_right(d)

        def pass_on(h0, h1):
            for way, h, t in ((0, h0, a), (1, h1, b)):
                ring_copy(way, d, h, t).wait_recv()

                @pl.when((d + 1 < far) | (h == way))
                def _():
                    ring_copy(way, d + 1, h, t).start()

                twin_copy(way, d, h, t).start()

        pass_on(0, 1)
        la, lb = from_left(d - 1) + other, from_right(d - 1) + other

        def earlier(k, carry):
            @pl.when(k == 0)
            def _():
                twin_ready(0, d - 1, la)

            @pl.when(k == 1)
            def _():
                twin_ready(1, d - 1, lb)

            process(la * (1 - k) + lb * k)
            return carry

        lax.fori_loop(0, jnp.minimum(d, 2), earlier, 0)
        pass_on(1, 0)

        def now(k, carry):
            process(a * (1 - k) + b * k)
            return carry

        lax.fori_loop(0, 2, now, 0)
        return carry

    lax.fori_loop(1, far, step, 0)

    last = from_left(far)
    for way in range(2):
        ring_copy(way, far, way, last).wait_recv()
        twin_copy(way, far, way, last).start()
    twin_ready(0, far - 1, from_left(far - 1) + other)
    twin_ready(1, far - 1, from_right(far - 1) + other)

    def tail(k, carry):
        @pl.when(k == 3)
        def _():
            for way in range(2):
                twin_copy(way, far, way, last + other).wait_recv()

        t = tile_at((pos + jnp.where(k == 0, R - far + 1, jnp.where(k == 1, far - 1, far))) % R, core)
        process(t + jnp.where(k == 2, 0, other))
        return carry

    lax.fori_loop(0, 4, tail, 0)

    pltpu.make_async_copy(
        all_local.at[pl.ds(0, N - 1)], all_local.at[pl.ds(0, N - 1)], stat_recv
    ).wait()
    logs = all_local[...].reshape(N, T)
    crest = jnp.max(logs, axis=0, keepdims=True)
    log_norm = crest + jnp.log(jnp.sum(jnp.exp(logs - crest), axis=0, keepdims=True))
    every_norm[me] = log_norm
    norm_ref[...] = log_norm

    def publish(i, carry):
        peer = (me + i) % G
        pltpu.make_async_remote_copy(
            src_ref=every_norm.at[me], dst_ref=every_norm.at[me],
            send_sem=norm_send, recv_sem=norm_recv,
            device_id={"pts": peer, "cen": cen}, device_id_type=MESH,
        ).start()
        return carry

    lax.fori_loop(1, G, publish, 0)
    group = every_norm.at[pl.ds(0, G - 1)]
    pltpu.make_async_copy(group, group, norm_recv).wait()

    def scale(t, carry):
        cols = pl.ds(pl.multiple_of(t * T, T), T)
        factor = jnp.exp(peaks[t] - every_norm[t])
        factors[:, cols] = jnp.broadcast_to(factor, (8, T))
        column = jnp.broadcast_to(factor, (8, T)).T[:, :1]
        pts_scaled[cols, :] = (pts_all[cols, :].astype(jnp.float32) * column).astype(jnp.bfloat16)
        return carry

    lax.fori_loop(0, G, scale, 0, unroll=8)

    KC = min(16, G) * W

    def update(r, carry):
        rows = pl.ds(pl.multiple_of(r * RB, RB), RB)

        def chunk(j, sums):
            weighted, mass = sums
            base = pl.multiple_of(j * KC * 128, KC * 128)
            parts = [shares[j * KC + g, rows, :] for g in range(KC)]
            weighted += jnp.dot(
                jnp.concatenate(parts, axis=1), pts_scaled[pl.ds(base, KC * 128), :],
                preferred_element_type=jnp.float32,
            )
            for g in range(KC):
                cols = pl.ds(pl.multiple_of(base + g * 128, 128), 128)
                mass += parts[g].astype(jnp.float32) * factors[:1, cols]
            return weighted, mass

        start = (jnp.zeros((RB, D), jnp.float32), jnp.zeros((RB, 128), jnp.float32))
        weighted, mass = lax.fori_loop(0, G * W // KC, chunk, start, unroll=True)
        total = prior_count + jnp.sum(mass, axis=1, keepdims=True)
        out_ref[rows, :] = (table[rows, :].astype(jnp.float32) + weighted) / total
        return carry

    lax.fori_loop(0, NB, update, 0, unroll=2 if NB % 2 == 0 else 1)

    sent = pts_all.at[pl.ds(0, (G - 1) * T)]
    pltpu.make_async_copy(sent, sent, send_sem).wait()
    pltpu.make_async_copy(
        all_local.at[pl.ds(0, N - 1)], all_local.at[pl.ds(0, N - 1)], stat_send
    ).wait()
    pltpu.make_async_copy(group, group, norm_send).wait()


def body(G, C, points, centroids):
    T, D = points.shape
    own = centroids.shape[0] // G
    far = G // 4
    updated, log_norm = pl.pallas_call(
        functools.partial(kernel, G, C),
        out_shape=(
            pltpu.VMEM((own, D), jnp.float32),
            jax.ShapeDtypeStruct((1, T), jnp.float32),
        ),
        in_specs=[pl.BlockSpec(memory_space=pl.ANY)] * 2,
        out_specs=(pl.BlockSpec(memory_space=pltpu.VMEM),) * 2,
        scratch_shapes=[
            pltpu.VMEM((G * T, D), jnp.bfloat16),
            pltpu.VMEM((G * T, D), jnp.bfloat16),
            pltpu.VMEM((own, D), jnp.bfloat16),
            pltpu.VMEM((own, T), jnp.float32),
            pltpu.VMEM((own, T), jnp.float32),
            pltpu.VMEM((G * T // 128, own, 128), jnp.bfloat16),
            pltpu.VMEM((G, 1, T), jnp.float32),
            pltpu.VMEM((G, 1, T), jnp.float32),
            pltpu.VMEM((G * C, 1, T), jnp.float32),
            pltpu.VMEM((G, 1, T), jnp.float32),
            pltpu.VMEM((8, G * T), jnp.float32),
            pltpu.SemaphoreType.DMA((2,)),
            pltpu.SemaphoreType.DMA,
            pltpu.SemaphoreType.DMA((2, far + 1, 2)),
            pltpu.SemaphoreType.DMA((2, far + 1, 2)),
            pltpu.SemaphoreType.DMA,
            pltpu.SemaphoreType.DMA,
            pltpu.SemaphoreType.DMA,
            pltpu.SemaphoreType.DMA,
        ],
        compiler_params=pltpu.CompilerParams(
            collective_id=0, has_side_effects=True, vmem_limit_bytes=60 * 1024 * 1024
        ),
    )(points, centroids)
    return updated, log_norm.reshape(T)


def solution(mesh):
    placed = (P("pts", None), P("cen", None))
    return jax.shard_map(
        functools.partial(body, mesh.shape["pts"], mesh.shape["cen"]),
        mesh=mesh,
        in_specs=placed,
        out_specs=(P(("cen", "pts"), None), P("pts")),
        check_vma=False,
    )
```

```python
import functools
import math

import jax
import jax.numpy as jnp
from jax import lax
from jax.experimental import pallas as pl
from jax.experimental.pallas import tpu as pltpu
from jax.sharding import PartitionSpec as P

inv_temp = 0.0625
prior_count = 1.0
log2e = math.log2(math.e)
MESH = pl.DeviceIdType.MESH
Q = 4


def kernel(
    G, C, L, points_ref, table_ref, out_ref, norm_ref,
    pts_all, pts_scaled, table, half_norms, scores, shares,
    tops, peaks, near, wide, factors,
    load_sem, send_sem, ring_sem, twin_sem, near_send, near_recv, wide_send, wide_recv,
):
    T, D = points_ref.shape
    own = table.shape[0]
    W = T // 128
    R = G // 2
    far = R // 2
    piece = T // Q
    H = G // L
    RB = min(256, own)
    NB = own // RB
    me = lax.axis_index("pts")
    cen = lax.axis_index("cen")
    core = me % 2
    chip = me // 2
    turn = chip % 2
    pos = (chip // 2) * (1 - turn) + (R - 1 - chip // 2) * turn
    other = 1 - 2 * core
    hi = me // L
    slot = (me % L) * C + cen

    def tile_at(p, c):
        s = p // far
        return ((1 - s) * 2 * p + s * (2 * (R - 1 - p) + 1)) * 2 + c

    twin = me + other
    right = tile_at((pos + 1) % R, core)
    left = tile_at((pos + R - 1) % R, core)

    my_points = pts_all.at[pl.ds(pl.multiple_of(me * T, T), T)]
    load_points = pltpu.make_async_copy(points_ref, my_points, load_sem.at[0])
    load_points.start()
    load_table = pltpu.make_async_copy(
        table_ref.at[pl.ds(pl.multiple_of(me * own, own), own)], table, load_sem.at[1]
    )
    load_table.start()

    barrier = pltpu.get_barrier_semaphore()

    for peer in (right, left, twin):
        pl.semaphore_signal(
            barrier, inc=1, device_id={"pts": peer, "cen": cen}, device_id_type=MESH
        )
    for i in range(1, C):
        pl.semaphore_signal(
            barrier, inc=1, device_id={"pts": me, "cen": (cen + i) % C}, device_id_type=MESH
        )
    load_points.wait()
    pl.semaphore_wait(barrier, 2 + C)

    def from_side(way, d):
        return tile_at((pos + R + (2 * way - 1) * d) % R, core)

    def rows_of(t, q):
        return pts_all.at[pl.ds(pl.multiple_of(t * T + q * piece, piece), piece)]

    def ring_copy(way, d, q, t):
        return pltpu.make_async_remote_copy(
            src_ref=rows_of(t, q), dst_ref=rows_of(t, q), send_sem=send_sem,
            recv_sem=ring_sem.at[way, d, q],
            device_id={"pts": (right, left)[way], "cen": cen}, device_id_type=MESH,
        )

    def twin_copy(way, d, q, t):
        return pltpu.make_async_remote_copy(
            src_ref=rows_of(t, q), dst_ref=rows_of(t, q), send_sem=send_sem,
            recv_sem=twin_sem.at[way, d, q],
            device_id={"pts": twin, "cen": cen}, device_id_type=MESH,
        )

    for i in range(Q):
        ring_copy(0, 1, i, me).start()
        ring_copy(1, 1, Q - 1 - i, me).start()
    for q in range(Q):
        twin_copy(0, 0, q, me).start()

    def pass_on(d, i):
        for way in range(2):
            q = i if way == 0 else Q - 1 - i
            t = from_side(way, d)
            ring_copy(way, d, q, t).wait_recv()

            @pl.when((d + 1 < far) | ((d + 1 == far) & (i < Q // 2)))
            def _():
                ring_copy(way, d + 1, q, t).start()

            twin_copy(way, d, q, t).start()

    load_table.wait()

    def norms(r, carry):
        rows = pl.ds(pl.multiple_of(r * RB, RB), RB)
        block = table[rows, :].astype(jnp.float32)
        total = jnp.sum(block * block, axis=1, keepdims=True)
        half_norms[rows, :] = jnp.broadcast_to(0.5 * total, (RB, 128))
        return carry

    lax.fori_loop(0, NB, norms, 0, unroll=2 if NB % 2 == 0 else 1)

    lowest = jnp.full((8, T), -jnp.inf, jnp.float32)

    def score(tile, r, top):
        rows = slice(r * RB, (r + 1) * RB)
        u = lax.dot_general(
            table[rows, :], tile, (((1,), (1,)), ((), ())),
            preferred_element_type=jnp.float32,
        ) - jnp.concatenate([half_norms[rows, :]] * W, axis=1)
        scores[rows, :] = u
        return jnp.maximum(top, jnp.max(u.reshape(RB // 8, 8, T), axis=0))

    def weigh(t, r, peak, total):
        rows = slice(r * RB, (r + 1) * RB)
        e = jnp.exp2((scores[rows, :] - peak) * (2.0 * inv_temp * log2e))
        packed = e.astype(jnp.bfloat16)
        for g in range(W):
            shares[t * W + g, rows, :] = packed[:, g * 128:(g + 1) * 128]
        return total + jnp.sum(e.reshape(RB // 8, 8, T), axis=0)

    def finish(t, peak, total):
        scaled = peak * (2.0 * inv_temp)
        peaks[pl.ds(t, 1), :] = scaled
        near[slot, pl.ds(t, 1), :] = scaled + jnp.log(jnp.sum(total, axis=0, keepdims=True))

    def points_of(t):
        return pts_all[pl.ds(pl.multiple_of(t * T, T), T), :]

    def first(t):
        tile = points_of(t)
        top = lowest
        for r in range(NB):
            top = score(tile, r, top)
        tops[...] = top

    def advance(before, t):
        peak = jnp.max(tops[...], axis=0, keepdims=True)
        tile = points_of(t)
        top, total = lowest, jnp.zeros((8, T), jnp.float32)
        for r in range(NB):
            total = weigh(before, r, peak, total)
            top = score(tile, r, top)
        tops[...] = top
        finish(before, peak, total)

    def last(t):
        peak = jnp.max(tops[...], axis=0, keepdims=True)
        total = jnp.zeros((8, T), jnp.float32)
        for r in range(NB):
            total = weigh(t, r, peak, total)
        finish(t, peak, total)

    first(me)
    for q in range(Q):
        twin_copy(0, 0, q, twin).wait_recv()
    advance(me, twin)
    for i in range(Q - 1):
        pass_on(1, i)

    def step(j, before):
        d, k = 1 + j // 4, j % 4

        @pl.when(k == 0)
        def _():
            pass_on(d, Q - 1)

        @pl.when((k > 0) & (d + 1 < far))
        def _():
            pass_on(d + 1, k - 1)

        @pl.when((k > 1) & (d + 1 == far))
        def _():
            pass_on(d + 1, k - 2)

        for way in range(2):
            @pl.when(k == 2 + way)
            def _():
                t = from_side(way, d) + other
                for q in range(Q):
                    twin_copy(way, d, q, t).wait_recv()

        side = k % 2
        t = from_side(0, d) * (1 - side) + from_side(1, d) * side
        t = t + jnp.where(k >= 2, other, 0)
        advance(before, t)
        return t

    before = lax.fori_loop(0, 4 * (far - 1), step, twin)
    end = from_side(0, far)
    advance(before, end)
    for i in range(Q // 2):
        twin_copy(0, far, i, end + other).wait_recv()
        twin_copy(1, far, Q - 1 - i, end + other).wait_recv()
    advance(end, end + other)
    last(end + other)

    def tell(i, carry):
        s = (slot + i) % (L * C)
        pltpu.make_async_remote_copy(
            src_ref=near.at[slot], dst_ref=near.at[slot],
            send_sem=near_send, recv_sem=near_recv,
            device_id={"pts": hi * L + s // C, "cen": s % C}, device_id_type=MESH,
        ).start()
        return carry

    lax.fori_loop(1, L * C, tell, 0)
    near_group = near.at[pl.ds(0, L * C - 1)]
    pltpu.make_async_copy(near_group, near_group, near_recv).wait()

    def merge(logs):
        crest = jnp.max(logs, axis=0)
        return crest + jnp.log(jnp.sum(jnp.exp(logs - crest[None]), axis=0))

    wide[hi] = merge(near[...])

    def spread(i, carry):
        h = (hi + i) % H
        pltpu.make_async_remote_copy(
            src_ref=wide.at[hi], dst_ref=wide.at[hi],
            send_sem=wide_send, recv_sem=wide_recv,
            device_id={"pts": h * L + me % L, "cen": cen}, device_id_type=MESH,
        ).start()
        return carry

    lax.fori_loop(1, H, spread, 0)
    wide_group = wide.at[pl.ds(0, H - 1)]
    pltpu.make_async_copy(wide_group, wide_group, wide_recv).wait()
    log_norm = merge(wide[...])
    factors[...] = log_norm
    norm_ref[...] = factors[pl.ds(me, 1), :]
    factors[...] = jnp.exp(peaks[...] - log_norm)

    def scale(j, carry):
        columns = factors[pl.ds(pl.multiple_of(j * 8, 8), 8), :].T
        for i in range(8):
            rows = pl.ds(pl.multiple_of((j * 8 + i) * T, T), T)
            pts_scaled[rows, :] = (
                pts_all[rows, :].astype(jnp.float32) * columns[:, i:i + 1]
            ).astype(jnp.bfloat16)
        return carry

    lax.fori_loop(0, G // 8, scale, 0)

    KC = min(16, G)

    def update(r, carry):
        rows = pl.ds(pl.multiple_of(r * RB, RB), RB)
        weighted = jnp.zeros((RB, D), jnp.float32)
        mass = jnp.zeros((RB, 128), jnp.float32)
        for j in range(G // KC):
            parts = [shares[j * KC * W + g, rows, :] for g in range(KC * W)]
            weighted += jnp.dot(
                jnp.concatenate(parts, axis=1), pts_scaled[j * KC * T:(j + 1) * KC * T, :],
                preferred_element_type=jnp.float32,
            )
            for g in range(KC * W):
                t, h = j * KC + g // W, g % W
                mass += parts[g].astype(jnp.float32) * factors[t:t + 1, h * 128:(h + 1) * 128]
        total = prior_count + jnp.sum(mass, axis=1, keepdims=True)
        out_ref[rows, :] = (table[rows, :].astype(jnp.float32) + weighted) / total
        return carry

    lax.fori_loop(0, NB, update, 0, unroll=2 if NB % 2 == 0 else 1)

    sent = pts_all.at[pl.ds(0, (G - 1) * T)]
    pltpu.make_async_copy(sent, sent, send_sem).wait()
    pltpu.make_async_copy(near_group, near_group, near_send).wait()
    pltpu.make_async_copy(wide_group, wide_group, wide_send).wait()


def body(G, C, points, centroids):
    T, D = points.shape
    own = centroids.shape[0] // G
    far = G // 4
    L = 1 << ((G.bit_length() - 1) // 2)
    H = G // L
    updated, log_norm = pl.pallas_call(
        functools.partial(kernel, G, C, L),
        out_shape=(
            pltpu.VMEM((own, D), jnp.float32),
            jax.ShapeDtypeStruct((1, T), jnp.float32),
        ),
        in_specs=[pl.BlockSpec(memory_space=pl.ANY)] * 2,
        out_specs=(pl.BlockSpec(memory_space=pltpu.VMEM),) * 2,
        scratch_shapes=[
            pltpu.VMEM((G * T, D), jnp.bfloat16),
            pltpu.VMEM((G * T, D), jnp.bfloat16),
            pltpu.VMEM((own, D), jnp.bfloat16),
            pltpu.VMEM((own, 128), jnp.float32),
            pltpu.VMEM((own, T), jnp.float32),
            pltpu.VMEM((G * T // 128, own, 128), jnp.bfloat16),
            pltpu.VMEM((8, T), jnp.float32),
            pltpu.VMEM((G, T), jnp.float32),
            pltpu.VMEM((L * C, G, T), jnp.float32),
            pltpu.VMEM((H, G, T), jnp.float32),
            pltpu.VMEM((G, T), jnp.float32),
            pltpu.SemaphoreType.DMA((2,)),
            pltpu.SemaphoreType.DMA,
            pltpu.SemaphoreType.DMA((2, far + 1, Q)),
            pltpu.SemaphoreType.DMA((2, far + 1, Q)),
            pltpu.SemaphoreType.DMA,
            pltpu.SemaphoreType.DMA,
            pltpu.SemaphoreType.DMA,
            pltpu.SemaphoreType.DMA,
        ],
        compiler_params=pltpu.CompilerParams(
            collective_id=0, has_side_effects=True, vmem_limit_bytes=60 * 1024 * 1024
        ),
    )(points, centroids)
    return updated, log_norm.reshape(T)


def solution(mesh):
    placed = (P("pts", None), P("cen", None))
    return jax.shard_map(
        functools.partial(body, mesh.shape["pts"], mesh.shape["cen"]),
        mesh=mesh,
        in_specs=placed,
        out_specs=(P(("cen", "pts"), None), P("pts")),
        check_vma=False,
    )
```

```python
import functools
import math

import jax
import jax.numpy as jnp
from jax import lax
from jax.experimental import pallas as pl
from jax.experimental.pallas import tpu as pltpu
from jax.sharding import PartitionSpec as P

inv_temp = 0.0625
prior_count = 1.0
log2e = math.log2(math.e)
MESH = pl.DeviceIdType.MESH
Q = 4
A = 3


def kernel(
    G, C, L, points_ref, table_ref, out_ref, norm_ref,
    pts_all, pts_scaled, tables, half_norms, scores, shares,
    tops, peaks, extra, near, wide, factors,
    load_sem, send_sem, ring_sem, twin_sem, near_send, near_recv, wide_send, wide_recv,
):
    T, D = points_ref.shape
    own = tables.shape[1]
    table = tables.at[A]
    W = T // 128
    R = G // 2
    far = R // 2
    piece = T // Q
    H = G // L
    RB = min(256, own)
    NB = own // RB
    me = lax.axis_index("pts")
    cen = lax.axis_index("cen")
    core = me % 2
    chip = me // 2
    turn = chip % 2
    pos = (chip // 2) * (1 - turn) + (R - 1 - chip // 2) * turn
    other = 1 - 2 * core
    hi = me // L
    slot = (me % L) * C + cen

    def tile_at(p, c):
        s = p // far
        return ((1 - s) * 2 * p + s * (2 * (R - 1 - p) + 1)) * 2 + c

    twin = me + other
    right = tile_at((pos + 1) % R, core)
    left = tile_at((pos + R - 1) % R, core)

    def from_side(way, d):
        return tile_at((pos + R + (2 * way - 1) * d) % R, core)

    my_points = pts_all.at[pl.ds(pl.multiple_of(me * T, T), T)]
    load_points = pltpu.make_async_copy(points_ref, my_points, load_sem.at[0])
    load_points.start()
    blocks = (from_side(0, far - 1), from_side(1, far - 1), from_side(0, far), me)
    loads = [
        pltpu.make_async_copy(
            table_ref.at[pl.ds(pl.multiple_of(block * own, own), own)],
            tables.at[j], load_sem.at[1 + j],
        )
        for j, block in enumerate(blocks)
    ]
    for load in loads:
        load.start()

    barrier = pltpu.get_barrier_semaphore()

    for peer in (right, left, twin):
        pl.semaphore_signal(
            barrier, inc=1, device_id={"pts": peer, "cen": cen}, device_id_type=MESH
        )
    for i in range(1, C):
        pl.semaphore_signal(
            barrier, inc=1, device_id={"pts": me, "cen": (cen + i) % C}, device_id_type=MESH
        )
    load_points.wait()
    pl.semaphore_wait(barrier, 2 + C)

    def rows_of(t, q):
        return pts_all.at[pl.ds(pl.multiple_of(t * T + q * piece, piece), piece)]

    def ring_copy(way, d, q, t):
        return pltpu.make_async_remote_copy(
            src_ref=rows_of(t, q), dst_ref=rows_of(t, q), send_sem=send_sem,
            recv_sem=ring_sem.at[way, d, q],
            device_id={"pts": (right, left)[way], "cen": cen}, device_id_type=MESH,
        )

    def twin_copy(way, d, q, t):
        return pltpu.make_async_remote_copy(
            src_ref=rows_of(t, q), dst_ref=rows_of(t, q), send_sem=send_sem,
            recv_sem=twin_sem.at[way, d, q],
            device_id={"pts": twin, "cen": cen}, device_id_type=MESH,
        )

    for i in range(Q):
        ring_copy(0, 1, i, me).start()
        ring_copy(1, 1, Q - 1 - i, me).start()
    for q in range(Q):
        twin_copy(0, 0, q, me).start()

    def pass_on(d, i):
        for way in range(2):
            q = i if way == 0 else Q - 1 - i
            t = from_side(way, d)
            ring_copy(way, d, q, t).wait_recv()

            @pl.when((d + 1 < far) | ((d + 1 == far) & (i < Q // 2)))
            def _():
                ring_copy(way, d + 1, q, t).start()

            twin_copy(way, d, q, t).start()

    near[slot] = jnp.full((G, T), -1e30, jnp.float32)

    def norms(j):
        def some(r, carry):
            rows = pl.ds(pl.multiple_of(r * RB, RB), RB)
            block = tables[j, rows, :].astype(jnp.float32)
            total = jnp.sum(block * block, axis=1, keepdims=True)
            half_norms[j % 2, rows, :] = jnp.broadcast_to(0.5 * total, (RB, 128))
            return carry

        lax.fori_loop(0, NB, some, 0, unroll=2 if NB % 2 == 0 else 1)

    lowest = jnp.full((8, T), -jnp.inf, jnp.float32)

    def score(j, tile, r, top):
        rows = slice(r * RB, (r + 1) * RB)
        u = lax.dot_general(
            tables[j, rows, :], tile, (((1,), (1,)), ((), ())),
            preferred_element_type=jnp.float32,
        ) - jnp.concatenate([half_norms[j % 2, rows, :]] * W, axis=1)
        scores[rows, :] = u
        return jnp.maximum(top, jnp.max(u.reshape(RB // 8, 8, T), axis=0))

    def weigh(t, r, peak, total):
        rows = slice(r * RB, (r + 1) * RB)
        e = jnp.exp2((scores[rows, :] - peak) * (2.0 * inv_temp * log2e))
        if t is not None:
            packed = e.astype(jnp.bfloat16)
            for g in range(W):
                shares[t * W + g, rows, :] = packed[:, g * 128:(g + 1) * 128]
        return total + jnp.sum(e.reshape(RB // 8, 8, T), axis=0)

    def finish(t, peak, total):
        scaled = peak * (2.0 * inv_temp)
        if t is not None:
            peaks[pl.ds(t, 1), :] = scaled
        return scaled + jnp.log(jnp.sum(total, axis=0, keepdims=True))

    def points_of(t):
        return pts_all[pl.ds(pl.multiple_of(t * T, T), T), :]

    def advance(before, j, t):
        tile = points_of(t)
        peak = jnp.max(tops[...], axis=0, keepdims=True)
        top, total = lowest, jnp.zeros((8, T), jnp.float32)
        for r in range(NB):
            total = weigh(before, r, peak, total)
            top = score(j, tile, r, top)
        tops[...] = top
        return finish(before, peak, total)

    def piece_on(m):
        pass_on(1 + m // Q, m % Q)

    loads[0].wait()
    norms(0)
    tile = points_of(me)
    top = lowest
    for r in range(NB):
        top = score(0, tile, r, top)
    tops[...] = top
    for q in range(Q):
        twin_copy(0, 0, q, twin).wait_recv()
    def borrow(j, carry):
        @pl.when(j > 0)
        def _():
            piece_on(2 * j - 1)

        extra[0, pl.ds(j, 1), :] = advance(None, j, twin)
        pltpu.make_async_copy(
            table_ref.at[pl.ds(0, own)], tables.at[j + 1], load_sem.at[j + 2]
        ).wait()
        norms(j + 1)
        piece_on(2 * j)
        extra[1, pl.ds(j, 1), :] = advance(None, j + 1, me)
        return carry

    lax.fori_loop(0, A, borrow, 0)
    piece_on(2 * A - 1)
    extra[0, A:A + 1, :] = advance(me, A, twin)

    def tile_of(d, k):
        side = k % 2
        t = from_side(0, d) * (1 - side) + from_side(1, d) * side
        return t + jnp.where(k >= 2, other, 0)

    def arrived(d, k, t):
        for way in range(2):
            @pl.when(k == 2 + way)
            def _():
                for q in range(Q):
                    twin_copy(way, d, q, t).wait_recv()

    def step(j, before):
        d, k = 1 + j // 4, j % 4
        t = tile_of(d, k)
        piece_on(j + 2 * A)
        arrived(d, k, t)
        value = advance(before, A, t)

        @pl.when(j == 0)
        def _():
            extra[1, A:A + 1, :] = value

        @pl.when(j > 0)
        def _():
            near[slot, pl.ds(before, 1), :] = value

        return t

    before = lax.fori_loop(0, 4 * (far - 2), step, twin)
    t = tile_of(far - 1, 0)
    near[slot, pl.ds(before, 1), :] = advance(before, A, t)
    for i, home in enumerate((me, twin)):
        parts = extra[i]
        crest = jnp.max(parts, axis=0, keepdims=True)
        near[slot, pl.ds(home, 1), :] = crest + jnp.log(
            jnp.sum(jnp.exp(parts - crest), axis=0, keepdims=True)
        )
    before = t

    def tell(i, carry):
        s = (slot + i) % (L * C)
        pltpu.make_async_remote_copy(
            src_ref=near.at[slot], dst_ref=near.at[slot],
            send_sem=near_send, recv_sem=near_recv,
            device_id={"pts": hi * L + s // C, "cen": s % C}, device_id_type=MESH,
        ).start()
        return carry

    lax.fori_loop(1, L * C, tell, 0)
    def distant(k, before):
        t = tile_of(far - 1, k)
        arrived(far - 1, k, t)
        advance(before, A, t)
        return t

    before = lax.fori_loop(1, 4, distant, before)
    end = from_side(0, far)
    advance(before, A, end)

    near_group = near.at[pl.ds(0, L * C - 1)]
    pltpu.make_async_copy(near_group, near_group, near_recv).wait()

    def merge(logs):
        crest = jnp.max(logs, axis=0)
        return crest + jnp.log(jnp.sum(jnp.exp(logs - crest[None]), axis=0))

    wide[hi] = merge(near[...])

    def spread(i, carry):
        h = (hi + i) % H
        pltpu.make_async_remote_copy(
            src_ref=wide.at[hi], dst_ref=wide.at[hi],
            send_sem=wide_send, recv_sem=wide_recv,
            device_id={"pts": h * L + me % L, "cen": cen}, device_id_type=MESH,
        ).start()
        return carry

    lax.fori_loop(1, H, spread, 0)
    for i in range(Q // 2):
        twin_copy(0, far, i, end + other).wait_recv()
        twin_copy(1, far, Q - 1 - i, end + other).wait_recv()
    advance(end, A, end + other)
    peak = jnp.max(tops[...], axis=0, keepdims=True)
    for r in range(NB):
        weigh(end + other, r, peak, jnp.zeros((8, T), jnp.float32))
    peaks[pl.ds(end + other, 1), :] = peak * (2.0 * inv_temp)

    wide_group = wide.at[pl.ds(0, H - 1)]
    pltpu.make_async_copy(wide_group, wide_group, wide_recv).wait()
    log_norm = merge(wide[...])
    factors[...] = log_norm
    norm_ref[...] = factors[pl.ds(me, 1), :]
    factors[...] = jnp.exp(peaks[...] - log_norm)

    def scale(j, carry):
        columns = factors[pl.ds(pl.multiple_of(j * 8, 8), 8), :].T
        for i in range(8):
            rows = pl.ds(pl.multiple_of((j * 8 + i) * T, T), T)
            pts_scaled[rows, :] = (
                pts_all[rows, :].astype(jnp.float32) * columns[:, i:i + 1]
            ).astype(jnp.bfloat16)
        return carry

    lax.fori_loop(0, G // 8, scale, 0)

    KC = min(16, G)

    def update(r, carry):
        rows = pl.ds(pl.multiple_of(r * RB, RB), RB)
        weighted = jnp.zeros((RB, D), jnp.float32)
        mass = jnp.zeros((RB, 128), jnp.float32)
        for j in range(G // KC):
            parts = [shares[j * KC * W + g, rows, :] for g in range(KC * W)]
            weighted += jnp.dot(
                jnp.concatenate(parts, axis=1), pts_scaled[j * KC * T:(j + 1) * KC * T, :],
                preferred_element_type=jnp.float32,
            )
            for g in range(KC * W):
                t, h = j * KC + g // W, g % W
                mass += parts[g].astype(jnp.float32) * factors[t:t + 1, h * 128:(h + 1) * 128]
        total = prior_count + jnp.sum(mass, axis=1, keepdims=True)
        out_ref[rows, :] = (table[rows, :].astype(jnp.float32) + weighted) / total
        return carry

    lax.fori_loop(0, NB, update, 0, unroll=2 if NB % 2 == 0 else 1)

    sent = pts_all.at[pl.ds(0, (G - 1) * T)]
    pltpu.make_async_copy(sent, sent, send_sem).wait()
    pltpu.make_async_copy(near_group, near_group, near_send).wait()
    pltpu.make_async_copy(wide_group, wide_group, wide_send).wait()


def body(G, C, points, centroids):
    T, D = points.shape
    own = centroids.shape[0] // G
    far = G // 4
    L = 1 << ((G.bit_length() - 1) // 2)
    H = G // L
    updated, log_norm = pl.pallas_call(
        functools.partial(kernel, G, C, L),
        out_shape=(
            pltpu.VMEM((own, D), jnp.float32),
            jax.ShapeDtypeStruct((1, T), jnp.float32),
        ),
        in_specs=[pl.BlockSpec(memory_space=pl.ANY)] * 2,
        out_specs=(pl.BlockSpec(memory_space=pltpu.VMEM),) * 2,
        scratch_shapes=[
            pltpu.VMEM((G * T, D), jnp.bfloat16),
            pltpu.VMEM((G * T, D), jnp.bfloat16),
            pltpu.VMEM((A + 1, own, D), jnp.bfloat16),
            pltpu.VMEM((2, own, 128), jnp.float32),
            pltpu.VMEM((own, T), jnp.float32),
            pltpu.VMEM((G * T // 128, own, 128), jnp.bfloat16),
            pltpu.VMEM((8, T), jnp.float32),
            pltpu.VMEM((G, T), jnp.float32),
            pltpu.VMEM((2, A + 1, T), jnp.float32),
            pltpu.VMEM((L * C, G, T), jnp.float32),
            pltpu.VMEM((H, G, T), jnp.float32),
            pltpu.VMEM((G, T), jnp.float32),
            pltpu.SemaphoreType.DMA((A + 2,)),
            pltpu.SemaphoreType.DMA,
            pltpu.SemaphoreType.DMA((2, far + 1, Q)),
            pltpu.SemaphoreType.DMA((2, far + 1, Q)),
            pltpu.SemaphoreType.DMA,
            pltpu.SemaphoreType.DMA,
            pltpu.SemaphoreType.DMA,
            pltpu.SemaphoreType.DMA,
        ],
        compiler_params=pltpu.CompilerParams(
            collective_id=0, has_side_effects=True, vmem_limit_bytes=60 * 1024 * 1024
        ),
    )(points, centroids)
    return updated, log_norm.reshape(T)


def solution(mesh):
    placed = (P("pts", None), P("cen", None))
    return jax.shard_map(
        functools.partial(body, mesh.shape["pts"], mesh.shape["cen"]),
        mesh=mesh,
        in_specs=placed,
        out_specs=(P(("cen", "pts"), None), P("pts")),
        check_vma=False,
    )
```

```python
import functools
import math

import jax
import jax.numpy as jnp
from jax import lax
from jax.experimental import pallas as pl
from jax.experimental.pallas import tpu as pltpu
from jax.sharding import PartitionSpec as P

inv_temp = 0.0625
prior_count = 1.0
log2e = math.log2(math.e)
MESH = pl.DeviceIdType.MESH
Q = 4
A = 3


def kernel(
    G, C, L, points_ref, table_ref, out_ref, norm_ref,
    pts_all, pts_scaled, tables, half_norms, scores, shares,
    tops, peaks, extra, near, wide, factors,
    load_sem, send_sem, ring_sem, twin_sem, near_send, near_recv, wide_send, wide_recv,
):
    T, D = points_ref.shape
    own = tables.shape[1]
    table = tables.at[A]
    W = T // 128
    R = G // 2
    far = R // 2
    piece = T // Q
    H = G // L
    RB = min(256, own)
    NB = own // RB
    me = lax.axis_index("pts")
    cen = lax.axis_index("cen")
    core = me % 2
    chip = me // 2
    turn = chip % 2
    pos = (chip // 2) * (1 - turn) + (R - 1 - chip // 2) * turn
    other = 1 - 2 * core
    hi = me // L
    slot = (me % L) * C + cen

    def tile_at(p, c):
        s = p // far
        return ((1 - s) * 2 * p + s * (2 * (R - 1 - p) + 1)) * 2 + c

    twin = me + other
    right = tile_at((pos + 1) % R, core)
    left = tile_at((pos + R - 1) % R, core)

    def from_side(way, d):
        return tile_at((pos + R + (2 * way - 1) * d) % R, core)

    my_points = pts_all.at[pl.ds(pl.multiple_of(me * T, T), T)]
    load_points = pltpu.make_async_copy(points_ref, my_points, load_sem.at[0])
    load_points.start()
    blocks = (from_side(0, far - 1), from_side(1, far - 1), from_side(0, far), me)
    loads = [
        pltpu.make_async_copy(
            table_ref.at[pl.ds(pl.multiple_of(block * own, own), own)],
            tables.at[j], load_sem.at[1 + j],
        )
        for j, block in enumerate(blocks)
    ]
    for load in loads:
        load.start()

    barrier = pltpu.get_barrier_semaphore()

    for peer in (right, left, twin):
        pl.semaphore_signal(
            barrier, inc=1, device_id={"pts": peer, "cen": cen}, device_id_type=MESH
        )
    for i in range(1, C):
        pl.semaphore_signal(
            barrier, inc=1, device_id={"pts": me, "cen": (cen + i) % C}, device_id_type=MESH
        )
    load_points.wait()
    pl.semaphore_wait(barrier, 2 + C)

    def rows_of(t, q):
        return pts_all.at[pl.ds(pl.multiple_of(t * T + q * piece, piece), piece)]

    def ring_copy(way, d, q, t):
        return pltpu.make_async_remote_copy(
            src_ref=rows_of(t, q), dst_ref=rows_of(t, q), send_sem=send_sem,
            recv_sem=ring_sem.at[way, d, q],
            device_id={"pts": (right, left)[way], "cen": cen}, device_id_type=MESH,
        )

    def twin_copy(way, d, q, t):
        return pltpu.make_async_remote_copy(
            src_ref=rows_of(t, q), dst_ref=rows_of(t, q), send_sem=send_sem,
            recv_sem=twin_sem.at[way, d, q],
            device_id={"pts": twin, "cen": cen}, device_id_type=MESH,
        )

    for i in range(Q):
        ring_copy(0, 1, i, me).start()
        ring_copy(1, 1, Q - 1 - i, me).start()
    for q in range(Q):
        twin_copy(0, 0, q, me).start()

    def pass_on(d, i):
        for way in range(2):
            q = i if way == 0 else Q - 1 - i
            t = from_side(way, d)
            ring_copy(way, d, q, t).wait_recv()

            @pl.when((d + 1 < far) | ((d + 1 == far) & (i < Q // 2)))
            def _():
                ring_copy(way, d + 1, q, t).start()

            twin_copy(way, d, q, t).start()

    near[slot] = jnp.full((G, T), -1e30, jnp.float32)

    lowest = jnp.full((8, T), -jnp.inf, jnp.float32)

    def score(j, tile, r, top, fresh):
        rows = slice(r * RB, (r + 1) * RB)
        block = tables[j, rows, :]
        if fresh:
            wide_block = block.astype(jnp.float32)
            total = jnp.sum(wide_block * wide_block, axis=1, keepdims=True)
            half_norms[rows, :] = jnp.broadcast_to(0.5 * total, (RB, 128))
        u = lax.dot_general(
            block, tile, (((1,), (1,)), ((), ())), preferred_element_type=jnp.float32
        ) - jnp.concatenate([half_norms[rows, :]] * W, axis=1)
        scores[rows, :] = u
        return jnp.maximum(top, jnp.max(u.reshape(RB // 8, 8, T), axis=0))

    def weigh(t, r, peak, total):
        rows = slice(r * RB, (r + 1) * RB)
        e = jnp.exp2((scores[rows, :] - peak) * (2.0 * inv_temp * log2e))
        if t is not None:
            packed = e.astype(jnp.bfloat16)
            for g in range(W):
                shares[t * W + g, rows, :] = packed[:, g * 128:(g + 1) * 128]
        return total + jnp.sum(e.reshape(RB // 8, 8, T), axis=0)

    def finish(t, peak, total):
        scaled = peak * (2.0 * inv_temp)
        if t is not None:
            peaks[pl.ds(t, 1), :] = scaled
        return scaled + jnp.log(jnp.sum(total, axis=0, keepdims=True))

    def points_of(t):
        return pts_all[pl.ds(pl.multiple_of(t * T, T), T), :]

    def advance(before, *then):
        top, values = tops[...], []
        for j, t, fresh in then:
            tile = points_of(t)
            peak = jnp.max(top, axis=0, keepdims=True)
            top, total = lowest, jnp.zeros((8, T), jnp.float32)
            for r in range(NB):
                total = weigh(before, r, peak, total)
                top = score(j, tile, r, top, fresh)
            values.append(finish(before, peak, total))
            before = None if before is None else t
        tops[...] = top
        return values

    def piece_on(m):
        pass_on(1 + m // Q, m % Q)

    loads[0].wait()
    tile = points_of(me)
    top = lowest
    for r in range(NB):
        top = score(0, tile, r, top, True)
    tops[...] = top
    for q in range(Q):
        twin_copy(0, 0, q, twin).wait_recv()

    def borrow(j, carry):
        @pl.when(j > 1)
        def _():
            piece_on(2 * j - 3)

        @pl.when(j > 0)
        def _():
            piece_on(2 * j - 2)

        pltpu.make_async_copy(
            table_ref.at[pl.ds(0, own)], tables.at[j + 1], load_sem.at[j + 2]
        ).wait()
        mine, twins = advance(None, (j, twin, False), (j + 1, me, True))
        extra[0, pl.ds(j, 1), :] = mine
        extra[1, pl.ds(j, 1), :] = twins
        return carry

    lax.fori_loop(0, A, borrow, 0)

    def tile_of(d, k):
        side = k % 2
        t = from_side(0, d) * (1 - side) + from_side(1, d) * side
        return t + jnp.where(k >= 2, other, 0)

    def arrived(d, k, t):
        for way in range(2):
            @pl.when(k == 2 + way)
            def _():
                for q in range(Q):
                    twin_copy(way, d, q, t).wait_recv()

    def step(p, before):
        piece_on(2 * p + 2 * A - 3)
        piece_on(2 * p + 2 * A - 2)
        j = 2 * p - 1
        d0, k0, d1, k1 = 1 + j // 4, (j + 4) % 4, 1 + (j + 1) // 4, (j + 1) % 4
        t0 = jnp.where(p == 0, twin, tile_of(d0, k0))
        t1 = tile_of(d1, k1)

        @pl.when(p > 0)
        def _():
            arrived(d0, k0, t0)

        arrived(d1, k1, t1)
        first, second = advance(before, (A, t0, False), (A, t1, False))

        @pl.when(p == 0)
        def _():
            extra[0, A:A + 1, :] = first
            extra[1, A:A + 1, :] = second

        @pl.when(p > 0)
        def _():
            near[slot, pl.ds(before, 1), :] = first
            near[slot, pl.ds(t0, 1), :] = second

        return t1

    before = lax.fori_loop(0, 2 * far - 3, step, me)
    for i, home in enumerate((me, twin)):
        parts = extra[i]
        crest = jnp.max(parts, axis=0, keepdims=True)
        near[slot, pl.ds(home, 1), :] = crest + jnp.log(
            jnp.sum(jnp.exp(parts - crest), axis=0, keepdims=True)
        )
    def tell(i, carry):
        s = (slot + i) % (L * C)
        pltpu.make_async_remote_copy(
            src_ref=near.at[slot], dst_ref=near.at[slot],
            send_sem=near_send, recv_sem=near_recv,
            device_id={"pts": hi * L + s // C, "cen": s % C}, device_id_type=MESH,
        ).start()
        return carry

    lax.fori_loop(1, L * C, tell, 0)
    piece_on(Q * (far - 1) + 1)
    for k in (1, 2):
        arrived(far - 1, k, tile_of(far - 1, k))
    second, third, fourth = (tile_of(far - 1, k) for k in (1, 2, 3))
    advance(before, (A, second, False), (A, third, False))
    end = from_side(0, far)
    arrived(far - 1, 3, fourth)
    advance(third, (A, fourth, False), (A, end, False))

    near_group = near.at[pl.ds(0, L * C - 1)]
    pltpu.make_async_copy(near_group, near_group, near_recv).wait()

    def merge(logs):
        crest = jnp.max(logs, axis=0)
        return crest + jnp.log(jnp.sum(jnp.exp(logs - crest[None]), axis=0))

    wide[hi] = merge(near[...])

    def spread(i, carry):
        h = (hi + i) % H
        pltpu.make_async_remote_copy(
            src_ref=wide.at[hi], dst_ref=wide.at[hi],
            send_sem=wide_send, recv_sem=wide_recv,
            device_id={"pts": h * L + me % L, "cen": cen}, device_id_type=MESH,
        ).start()
        return carry

    lax.fori_loop(1, H, spread, 0)
    for i in range(Q // 2):
        twin_copy(0, far, i, end + other).wait_recv()
        twin_copy(1, far, Q - 1 - i, end + other).wait_recv()
    advance(end, (A, end + other, False))
    peak = jnp.max(tops[...], axis=0, keepdims=True)
    for r in range(NB):
        weigh(end + other, r, peak, jnp.zeros((8, T), jnp.float32))
    peaks[pl.ds(end + other, 1), :] = peak * (2.0 * inv_temp)

    wide_group = wide.at[pl.ds(0, H - 1)]
    pltpu.make_async_copy(wide_group, wide_group, wide_recv).wait()
    log_norm = merge(wide[...])
    factors[...] = log_norm
    norm_ref[...] = factors[pl.ds(me, 1), :]
    factors[...] = jnp.exp(peaks[...] - log_norm)

    def scale(j, carry):
        columns = factors[pl.ds(pl.multiple_of(j * 8, 8), 8), :].T
        for i in range(8):
            rows = pl.ds(pl.multiple_of((j * 8 + i) * T, T), T)
            pts_scaled[rows, :] = (
                pts_all[rows, :].astype(jnp.float32) * columns[:, i:i + 1]
            ).astype(jnp.bfloat16)
        return carry

    lax.fori_loop(0, G // 8, scale, 0)

    KC = min(16, G)

    def update(r, carry):
        rows = pl.ds(pl.multiple_of(r * RB, RB), RB)
        weighted = jnp.zeros((RB, D), jnp.float32)
        mass = jnp.zeros((RB, 128), jnp.float32)
        for j in range(G // KC):
            parts = [shares[j * KC * W + g, rows, :] for g in range(KC * W)]
            weighted += jnp.dot(
                jnp.concatenate(parts, axis=1), pts_scaled[j * KC * T:(j + 1) * KC * T, :],
                preferred_element_type=jnp.float32,
            )
            for g in range(KC * W):
                t, h = j * KC + g // W, g % W
                mass += parts[g].astype(jnp.float32) * factors[t:t + 1, h * 128:(h + 1) * 128]
        total = prior_count + jnp.sum(mass, axis=1, keepdims=True)
        out_ref[rows, :] = (table[rows, :].astype(jnp.float32) + weighted) / total
        return carry

    lax.fori_loop(0, NB, update, 0, unroll=2 if NB % 2 == 0 else 1)

    sent = pts_all.at[pl.ds(0, (G - 1) * T)]
    pltpu.make_async_copy(sent, sent, send_sem).wait()
    pltpu.make_async_copy(near_group, near_group, near_send).wait()
    pltpu.make_async_copy(wide_group, wide_group, wide_send).wait()


def body(G, C, points, centroids):
    T, D = points.shape
    own = centroids.shape[0] // G
    far = G // 4
    L = 1 << ((G.bit_length() - 1) // 2)
    H = G // L
    updated, log_norm = pl.pallas_call(
        functools.partial(kernel, G, C, L),
        out_shape=(
            pltpu.VMEM((own, D), jnp.float32),
            jax.ShapeDtypeStruct((1, T), jnp.float32),
        ),
        in_specs=[pl.BlockSpec(memory_space=pl.ANY)] * 2,
        out_specs=(pl.BlockSpec(memory_space=pltpu.VMEM),) * 2,
        scratch_shapes=[
            pltpu.VMEM((G * T, D), jnp.bfloat16),
            pltpu.VMEM((G * T, D), jnp.bfloat16),
            pltpu.VMEM((A + 1, own, D), jnp.bfloat16),
            pltpu.VMEM((own, 128), jnp.float32),
            pltpu.VMEM((own, T), jnp.float32),
            pltpu.VMEM((G * T // 128, own, 128), jnp.bfloat16),
            pltpu.VMEM((8, T), jnp.float32),
            pltpu.VMEM((G, T), jnp.float32),
            pltpu.VMEM((2, A + 1, T), jnp.float32),
            pltpu.VMEM((L * C, G, T), jnp.float32),
            pltpu.VMEM((H, G, T), jnp.float32),
            pltpu.VMEM((G, T), jnp.float32),
            pltpu.SemaphoreType.DMA((A + 2,)),
            pltpu.SemaphoreType.DMA,
            pltpu.SemaphoreType.DMA((2, far + 1, Q)),
            pltpu.SemaphoreType.DMA((2, far + 1, Q)),
            pltpu.SemaphoreType.DMA,
            pltpu.SemaphoreType.DMA,
            pltpu.SemaphoreType.DMA,
            pltpu.SemaphoreType.DMA,
        ],
        compiler_params=pltpu.CompilerParams(
            collective_id=0, has_side_effects=True, vmem_limit_bytes=60 * 1024 * 1024
        ),
    )(points, centroids)
    return updated, log_norm.reshape(T)


def solution(mesh):
    placed = (P("pts", None), P("cen", None))
    return jax.shard_map(
        functools.partial(body, mesh.shape["pts"], mesh.shape["cen"]),
        mesh=mesh,
        in_specs=placed,
        out_specs=(P(("cen", "pts"), None), P("pts")),
        check_vma=False,
    )
```

```python
import functools
import math

import jax
import jax.numpy as jnp
from jax import lax
from jax.experimental import pallas as pl
from jax.experimental.pallas import tpu as pltpu
from jax.sharding import PartitionSpec as P

inv_temp = 0.0625
prior_count = 1.0
log2e = math.log2(math.e)
MESH = pl.DeviceIdType.MESH
Q = 2
A = 3


def kernel(
    G, C, L, points_ref, table_ref, out_ref, norm_ref,
    pts_all, pts_scaled, tables, half_norms, scores, shares,
    tops, peaks, extra, near, wide, factors,
    load_sem, send_sem, ring_sem, twin_sem, near_send, near_recv, wide_send, wide_recv,
):
    T, D = points_ref.shape
    own = tables.shape[1]
    table = tables.at[A]
    W = T // 128
    R = G // 2
    far = R // 2
    piece = T // Q
    shift = Q.bit_length() - 1
    H = G // L
    RB = min(256, own)
    NB = own // RB
    RS = min(1024, own)
    NS = own // RS
    me = lax.axis_index("pts")
    cen = lax.axis_index("cen")
    core = me % 2
    chip = me // 2
    turn = chip % 2
    pos = (chip // 2) * (1 - turn) + (R - 1 - chip // 2) * turn
    other = 1 - 2 * core
    hi = me // L
    slot = (me % L) * C + cen

    def tile_at(p, c):
        return jnp.where(p < far, 2 * p, 2 * (R - 1 - p) + 1) * 2 + c

    twin = me + other
    right = tile_at((pos + 1) % R, core)
    left = tile_at((pos + R - 1) % R, core)

    def around(p):
        return p & (R - 1) if R & (R - 1) == 0 else lax.rem(p, R)

    def from_side(way, d):
        return tile_at(around(pos + R + (2 * way - 1) * d), core)

    my_points = pts_all.at[pl.ds(pl.multiple_of(me * T, T), T)]
    load_points = pltpu.make_async_copy(points_ref, my_points, load_sem.at[0])
    load_points.start()
    blocks = (from_side(0, far - 1), from_side(1, far - 1), from_side(0, far), me)
    loads = [
        pltpu.make_async_copy(
            table_ref.at[pl.ds(pl.multiple_of(block * own, own), own)],
            tables.at[j], load_sem.at[1 + j],
        )
        for j, block in enumerate(blocks)
    ]
    for load in loads:
        load.start()

    barrier = pltpu.get_barrier_semaphore()

    for peer in (right, left, twin):
        pl.semaphore_signal(
            barrier, inc=1, device_id={"pts": peer, "cen": cen}, device_id_type=MESH
        )
    for i in range(1, C):
        for peer in (me, twin):
            pl.semaphore_signal(
                barrier, inc=1, device_id={"pts": peer, "cen": (cen + i) % C}, device_id_type=MESH
            )
    load_points.wait()
    pl.semaphore_wait(barrier, 1 + 2 * C)

    def rows_of(t, q):
        return pts_all.at[pl.ds(pl.multiple_of(t * T + q * piece, piece), piece)]

    def ring_copy(way, d, q, t):
        return pltpu.make_async_remote_copy(
            src_ref=rows_of(t, q), dst_ref=rows_of(t, q), send_sem=send_sem,
            recv_sem=ring_sem.at[way, d, q],
            device_id={"pts": (right, left)[way], "cen": cen}, device_id_type=MESH,
        )

    def twin_copy(way, d, q, t):
        return pltpu.make_async_remote_copy(
            src_ref=rows_of(t, q), dst_ref=rows_of(t, q), send_sem=send_sem,
            recv_sem=twin_sem.at[way, d, q],
            device_id={"pts": twin, "cen": cen}, device_id_type=MESH,
        )

    for i in range(Q):
        ring_copy(0, 1, i, me).start()
        ring_copy(1, 1, Q - 1 - i, me).start()
    for q in range(Q):
        twin_copy(0, 0, q, me).start()

    def pass_on(d, i):
        for way in range(2):
            q = i if way == 0 else Q - 1 - i
            t = from_side(way, d)
            ring_copy(way, d, q, t).wait_recv()

            @pl.when((d + 1 < far) | ((d + 1 == far) & (i < Q // 2)))
            def _():
                ring_copy(way, d + 1, q, t).start()

            twin_copy(way, d, q, t).start()

    near[slot] = jnp.full((G, T), -1e30, jnp.float32)

    lowest = jnp.full((8, T), -jnp.inf, jnp.float32)

    def score(j, tile, r, top, fresh):
        rows = slice(r * RS, (r + 1) * RS)
        block = tables[j, rows, :]
        if fresh:
            wide_block = block.astype(jnp.float32)
            total = jnp.sum(wide_block * wide_block, axis=1, keepdims=True)
            half_norms[rows, :] = jnp.broadcast_to(0.5 * total, (RS, 128))
        u = lax.dot_general(
            block, tile, (((1,), (1,)), ((), ())), preferred_element_type=jnp.float32
        ) - jnp.concatenate([half_norms[rows, :]] * W, axis=1)
        scores[rows, :] = u
        return jnp.maximum(top, jnp.max(u.reshape(RS // 8, 8, T), axis=0))

    def weigh(t, r, peak, total):
        rows = slice(r * RS, (r + 1) * RS)
        e = jnp.exp2((scores[rows, :] - peak) * (2.0 * inv_temp * log2e))
        if t is not None:
            packed = e.astype(jnp.bfloat16)
            for g in range(W):
                shares[t * W + g, rows, :] = packed[:, g * 128:(g + 1) * 128]
        return total + jnp.sum(e.reshape(RS // 8, 8, T), axis=0)

    def finish(t, peak, total):
        scaled = peak * (2.0 * inv_temp)
        if t is not None:
            peaks[pl.ds(t, 1), :] = scaled
        return scaled + jnp.log(jnp.sum(total, axis=0, keepdims=True))

    def points_of(t):
        return pts_all[pl.ds(pl.multiple_of(t * T, T), T), :]

    def advance(before, *then):
        top, values = tops[...], []
        for j, t, fresh in then:
            tile = points_of(t)
            peak = jnp.max(top, axis=0, keepdims=True)
            top, total = lowest, jnp.zeros((8, T), jnp.float32)
            for r in range(NS):
                total = weigh(before, r, peak, total)
                top = score(j, tile, r, top, fresh)
            values.append(finish(before, peak, total))
            before = None if before is None else t
        tops[...] = top
        return values

    def piece_on(m):
        pass_on(1 + (m >> shift), m & (Q - 1))

    loads[0].wait()
    tile = points_of(me)
    top = lowest
    for r in range(NS):
        top = score(0, tile, r, top, True)
    tops[...] = top
    for q in range(Q):
        twin_copy(0, 0, q, twin).wait_recv()

    def borrow(j, carry):
        @pl.when(j > 1)
        def _():
            piece_on(j - 2)

        pltpu.make_async_copy(
            table_ref.at[pl.ds(0, own)], tables.at[j + 1], load_sem.at[j + 2]
        ).wait()
        mine, twins = advance(None, (j, twin, False), (j + 1, me, True))
        extra[0, pl.ds(j, 1), :] = mine
        extra[1, pl.ds(j, 1), :] = twins
        return carry

    lax.fori_loop(0, A, borrow, 0)

    def tile_of(d, k):
        side = k & 1
        t = from_side(0, d) * (1 - side) + from_side(1, d) * side
        return t + jnp.where(k >= 2, other, 0)

    def arrived(d, k, t):
        for way in range(2):
            @pl.when(k == 2 + way)
            def _():
                for q in range(Q):
                    twin_copy(way, d, q, t).wait_recv()

    def step(p, before):
        piece_on(p + A - 2)
        j = 2 * p - 1
        d0, k0, d1, k1 = 1 + (j >> 2), j & 3, 1 + ((j + 1) >> 2), (j + 1) & 3
        t0 = jnp.where(p == 0, twin, tile_of(d0, k0))
        t1 = tile_of(d1, k1)

        @pl.when(p > 0)
        def _():
            arrived(d0, k0, t0)

        arrived(d1, k1, t1)
        first, second = advance(before, (A, t0, False), (A, t1, False))

        @pl.when(p == 0)
        def _():
            extra[0, A:A + 1, :] = first
            extra[1, A:A + 1, :] = second

        @pl.when(p > 0)
        def _():
            near[slot, pl.ds(before, 1), :] = first
            near[slot, pl.ds(t0, 1), :] = second

        return t1

    before = lax.fori_loop(0, 2 * far - 3, step, me)
    for i, home in enumerate((me, twin)):
        parts = extra[i]
        crest = jnp.max(parts, axis=0, keepdims=True)
        near[slot, pl.ds(home, 1), :] = crest + jnp.log(
            jnp.sum(jnp.exp(parts - crest), axis=0, keepdims=True)
        )
    def tell(i, carry):
        s = (slot + i) % (L * C)
        pltpu.make_async_remote_copy(
            src_ref=near.at[slot], dst_ref=near.at[slot],
            send_sem=near_send, recv_sem=near_recv,
            device_id={"pts": hi * L + s // C, "cen": s % C}, device_id_type=MESH,
        ).start()
        return carry

    lax.fori_loop(1, L * C, tell, 0)
    piece_on(Q * (far - 1))
    for k in (1, 2):
        arrived(far - 1, k, tile_of(far - 1, k))
    second, third, fourth = (tile_of(far - 1, k) for k in (1, 2, 3))
    advance(before, (A, second, False), (A, third, False))
    end = from_side(0, far)
    arrived(far - 1, 3, fourth)
    advance(third, (A, fourth, False), (A, end, False))

    near_group = near.at[pl.ds(0, L * C - 1)]
    pltpu.make_async_copy(near_group, near_group, near_recv).wait()

    def merge(logs):
        crest = jnp.max(logs, axis=0)
        return crest + jnp.log(jnp.sum(jnp.exp(logs - crest[None]), axis=0))

    wide[hi] = merge(near[...])

    def spread(i, carry):
        h = (hi + i) % H
        pltpu.make_async_remote_copy(
            src_ref=wide.at[hi], dst_ref=wide.at[hi],
            send_sem=wide_send, recv_sem=wide_recv,
            device_id={"pts": h * L + me % L, "cen": cen}, device_id_type=MESH,
        ).start()
        return carry

    lax.fori_loop(1, H, spread, 0)
    for i in range(Q // 2):
        twin_copy(0, far, i, end + other).wait_recv()
        twin_copy(1, far, Q - 1 - i, end + other).wait_recv()
    advance(end, (A, end + other, False))
    peak = jnp.max(tops[...], axis=0, keepdims=True)
    for r in range(NS):
        weigh(end + other, r, peak, jnp.zeros((8, T), jnp.float32))
    peaks[pl.ds(end + other, 1), :] = peak * (2.0 * inv_temp)

    wide_group = wide.at[pl.ds(0, H - 1)]
    pltpu.make_async_copy(wide_group, wide_group, wide_recv).wait()
    log_norm = merge(wide[...])
    factors[...] = log_norm
    norm_ref[...] = factors[pl.ds(me, 1), :]
    factors[...] = jnp.exp(peaks[...] - log_norm)

    def scale(j, carry):
        columns = factors[pl.ds(pl.multiple_of(j * 8, 8), 8), :].T
        for i in range(8):
            rows = pl.ds(pl.multiple_of((j * 8 + i) * T, T), T)
            pts_scaled[rows, :] = (
                pts_all[rows, :].astype(jnp.float32) * columns[:, i:i + 1]
            ).astype(jnp.bfloat16)
        return carry

    lax.fori_loop(0, G // 8, scale, 0)

    KC = min(16, G)

    def update(r, carry):
        rows = pl.ds(pl.multiple_of(r * RB, RB), RB)
        weighted = jnp.zeros((RB, D), jnp.float32)
        mass = jnp.zeros((RB, 128), jnp.float32)
        for j in range(G // KC):
            parts = [shares[j * KC * W + g, rows, :] for g in range(KC * W)]
            weighted += jnp.dot(
                jnp.concatenate(parts, axis=1), pts_scaled[j * KC * T:(j + 1) * KC * T, :],
                preferred_element_type=jnp.float32,
            )
            for g in range(KC * W):
                t, h = j * KC + g // W, g % W
                mass += parts[g].astype(jnp.float32) * factors[t:t + 1, h * 128:(h + 1) * 128]
        total = prior_count + jnp.sum(mass, axis=1, keepdims=True)
        out_ref[rows, :] = (table[rows, :].astype(jnp.float32) + weighted) / total
        return carry

    lax.fori_loop(0, NB, update, 0, unroll=2 if NB % 2 == 0 else 1)

    sent = pts_all.at[pl.ds(0, (G - 1) * T)]
    pltpu.make_async_copy(sent, sent, send_sem).wait()
    pltpu.make_async_copy(near_group, near_group, near_send).wait()
    pltpu.make_async_copy(wide_group, wide_group, wide_send).wait()


def body(G, C, points, centroids):
    T, D = points.shape
    own = centroids.shape[0] // G
    far = G // 4
    L = 1 << ((G.bit_length() - 1) // 2)
    H = G // L
    updated, log_norm = pl.pallas_call(
        functools.partial(kernel, G, C, L),
        out_shape=(
            pltpu.VMEM((own, D), jnp.float32),
            jax.ShapeDtypeStruct((1, T), jnp.float32),
        ),
        in_specs=[pl.BlockSpec(memory_space=pl.ANY)] * 2,
        out_specs=(pl.BlockSpec(memory_space=pltpu.VMEM),) * 2,
        scratch_shapes=[
            pltpu.VMEM((G * T, D), jnp.bfloat16),
            pltpu.VMEM((G * T, D), jnp.bfloat16),
            pltpu.VMEM((A + 1, own, D), jnp.bfloat16),
            pltpu.VMEM((own, 128), jnp.float32),
            pltpu.VMEM((own, T), jnp.float32),
            pltpu.VMEM((G * T // 128, own, 128), jnp.bfloat16),
            pltpu.VMEM((8, T), jnp.float32),
            pltpu.VMEM((G, T), jnp.float32),
            pltpu.VMEM((2, A + 1, T), jnp.float32),
            pltpu.VMEM((L * C, G, T), jnp.float32),
            pltpu.VMEM((H, G, T), jnp.float32),
            pltpu.VMEM((G, T), jnp.float32),
            pltpu.SemaphoreType.DMA((A + 2,)),
            pltpu.SemaphoreType.DMA,
            pltpu.SemaphoreType.DMA((2, far + 1, Q)),
            pltpu.SemaphoreType.DMA((2, far + 1, Q)),
            pltpu.SemaphoreType.DMA,
            pltpu.SemaphoreType.DMA,
            pltpu.SemaphoreType.DMA,
            pltpu.SemaphoreType.DMA,
        ],
        compiler_params=pltpu.CompilerParams(
            collective_id=0, has_side_effects=True, vmem_limit_bytes=60 * 1024 * 1024
        ),
    )(points, centroids)
    return updated, log_norm.reshape(T)


def solution(mesh):
    placed = (P("pts", None), P("cen", None))
    return jax.shard_map(
        functools.partial(body, mesh.shape["pts"], mesh.shape["cen"]),
        mesh=mesh,
        in_specs=placed,
        out_specs=(P(("cen", "pts"), None), P("pts")),
        check_vma=False,
    )
```

```python
import functools
import math

import jax
import jax.numpy as jnp
from jax import lax
from jax.experimental import pallas as pl
from jax.experimental.pallas import tpu as pltpu
from jax.sharding import PartitionSpec as P

inv_temp = 0.0625
prior_count = 1.0
log2e = math.log2(math.e)
MESH = pl.DeviceIdType.MESH
Q = 2
A = 3


def kernel(
    G, C, L, points_ref, table_ref, shares, pts_scaled, factors, norm_ref, tables,
    pts_all, half_norms, scores,
    tops, peaks, extra, near, wide,
    load_sem, send_sem, ring_sem, twin_sem, near_send, near_recv, wide_send, wide_recv,
):
    T, D = points_ref.shape
    own = tables.shape[1]
    W = T // 128
    R = G // 2
    far = R // 2
    piece = T // Q
    shift = Q.bit_length() - 1
    H = G // L
    RS = min(1024, own)
    NS = own // RS
    me = lax.axis_index("pts")
    cen = lax.axis_index("cen")
    core = me % 2
    chip = me // 2
    turn = chip % 2
    pos = (chip // 2) * (1 - turn) + (R - 1 - chip // 2) * turn
    other = 1 - 2 * core
    hi = me // L
    slot = (me % L) * C + cen

    def tile_at(p, c):
        return jnp.where(p < far, 2 * p, 2 * (R - 1 - p) + 1) * 2 + c

    twin = me + other
    right = tile_at((pos + 1) % R, core)
    left = tile_at((pos + R - 1) % R, core)

    def around(p):
        return p & (R - 1) if R & (R - 1) == 0 else lax.rem(p, R)

    def from_side(way, d):
        return tile_at(around(pos + R + (2 * way - 1) * d), core)

    my_points = pts_all.at[pl.ds(pl.multiple_of(me * T, T), T)]
    load_points = pltpu.make_async_copy(points_ref, my_points, load_sem.at[0])
    load_points.start()
    blocks = (from_side(0, far - 1), from_side(1, far - 1), from_side(0, far), me)
    loads = [
        pltpu.make_async_copy(
            table_ref.at[pl.ds(pl.multiple_of(block * own, own), own)],
            tables.at[j], load_sem.at[1 + j],
        )
        for j, block in enumerate(blocks)
    ]
    for load in loads:
        load.start()

    barrier = pltpu.get_barrier_semaphore()

    for peer in (right, left, twin):
        pl.semaphore_signal(
            barrier, inc=1, device_id={"pts": peer, "cen": cen}, device_id_type=MESH
        )
    for i in range(1, C):
        for peer in (me, twin):
            pl.semaphore_signal(
                barrier, inc=1, device_id={"pts": peer, "cen": (cen + i) % C}, device_id_type=MESH
            )
    load_points.wait()
    pl.semaphore_wait(barrier, 1 + 2 * C)

    def rows_of(t, q):
        return pts_all.at[pl.ds(pl.multiple_of(t * T + q * piece, piece), piece)]

    def ring_copy(way, d, q, t):
        return pltpu.make_async_remote_copy(
            src_ref=rows_of(t, q), dst_ref=rows_of(t, q), send_sem=send_sem,
            recv_sem=ring_sem.at[way, d, q],
            device_id={"pts": (right, left)[way], "cen": cen}, device_id_type=MESH,
        )

    def twin_copy(way, d, q, t):
        return pltpu.make_async_remote_copy(
            src_ref=rows_of(t, q), dst_ref=rows_of(t, q), send_sem=send_sem,
            recv_sem=twin_sem.at[way, d, q],
            device_id={"pts": twin, "cen": cen}, device_id_type=MESH,
        )

    for i in range(Q):
        ring_copy(0, 1, i, me).start()
        ring_copy(1, 1, Q - 1 - i, me).start()
    for q in range(Q):
        twin_copy(0, 0, q, me).start()

    def pass_on(d, i):
        for way in range(2):
            q = i if way == 0 else Q - 1 - i
            t = from_side(way, d)
            ring_copy(way, d, q, t).wait_recv()

            @pl.when((d + 1 < far) | ((d + 1 == far) & (i < Q // 2)))
            def _():
                ring_copy(way, d + 1, q, t).start()

            twin_copy(way, d, q, t).start()

    near[slot] = jnp.full((G, T), -1e30, jnp.float32)

    lowest = jnp.full((8, T), -jnp.inf, jnp.float32)

    def score(j, tile, r, top, fresh):
        rows = slice(r * RS, (r + 1) * RS)
        block = tables[j, rows, :]
        if fresh:
            wide_block = block.astype(jnp.float32)
            total = jnp.sum(wide_block * wide_block, axis=1, keepdims=True)
            half_norms[rows, :] = jnp.broadcast_to(0.5 * total, (RS, 128))
        u = lax.dot_general(
            block, tile, (((1,), (1,)), ((), ())), preferred_element_type=jnp.float32
        ) - jnp.concatenate([half_norms[rows, :]] * W, axis=1)
        scores[rows, :] = u
        return jnp.maximum(top, jnp.max(u.reshape(RS // 8, 8, T), axis=0))

    def weigh(t, r, peak, total):
        rows = slice(r * RS, (r + 1) * RS)
        e = jnp.exp2((scores[rows, :] - peak) * (2.0 * inv_temp * log2e))
        if t is not None:
            packed = e.astype(jnp.bfloat16)
            for g in range(W):
                shares[t * W + g, rows, :] = packed[:, g * 128:(g + 1) * 128]
        return total + jnp.sum(e.reshape(RS // 8, 8, T), axis=0)

    def finish(t, peak, total):
        scaled = peak * (2.0 * inv_temp)
        if t is not None:
            peaks[pl.ds(t, 1), :] = scaled
        return scaled + jnp.log(jnp.sum(total, axis=0, keepdims=True))

    def points_of(t):
        return pts_all[pl.ds(pl.multiple_of(t * T, T), T), :]

    def advance(before, *then):
        top, values = tops[...], []
        for j, t, fresh in then:
            tile = points_of(t)
            peak = jnp.max(top, axis=0, keepdims=True)
            top, total = lowest, jnp.zeros((8, T), jnp.float32)
            for r in range(NS):
                total = weigh(before, r, peak, total)
                top = score(j, tile, r, top, fresh)
            values.append(finish(before, peak, total))
            before = None if before is None else t
        tops[...] = top
        return values

    def piece_on(m):
        pass_on(1 + (m >> shift), m & (Q - 1))

    loads[0].wait()
    tile = points_of(me)
    top = lowest
    for r in range(NS):
        top = score(0, tile, r, top, True)
    tops[...] = top
    for q in range(Q):
        twin_copy(0, 0, q, twin).wait_recv()

    def borrow(j, carry):
        @pl.when(j > 1)
        def _():
            piece_on(j - 2)

        pltpu.make_async_copy(
            table_ref.at[pl.ds(0, own)], tables.at[j + 1], load_sem.at[j + 2]
        ).wait()
        mine, twins = advance(None, (j, twin, False), (j + 1, me, True))
        extra[0, pl.ds(j, 1), :] = mine
        extra[1, pl.ds(j, 1), :] = twins
        return carry

    lax.fori_loop(0, A, borrow, 0)

    def tile_of(d, k):
        side = k & 1
        t = from_side(0, d) * (1 - side) + from_side(1, d) * side
        return t + jnp.where(k >= 2, other, 0)

    def arrived(d, k, t):
        for way in range(2):
            @pl.when(k == 2 + way)
            def _():
                for q in range(Q):
                    twin_copy(way, d, q, t).wait_recv()

    def step(p, before):
        piece_on(p + A - 2)
        j = 2 * p - 1
        d0, k0, d1, k1 = 1 + (j >> 2), j & 3, 1 + ((j + 1) >> 2), (j + 1) & 3
        t0 = jnp.where(p == 0, twin, tile_of(d0, k0))
        t1 = tile_of(d1, k1)

        @pl.when(p > 0)
        def _():
            arrived(d0, k0, t0)

        arrived(d1, k1, t1)
        first, second = advance(before, (A, t0, False), (A, t1, False))

        @pl.when(p == 0)
        def _():
            extra[0, A:A + 1, :] = first
            extra[1, A:A + 1, :] = second

        @pl.when(p > 0)
        def _():
            near[slot, pl.ds(before, 1), :] = first
            near[slot, pl.ds(t0, 1), :] = second

        return t1

    before = lax.fori_loop(0, 2 * far - 3, step, me)
    for i, home in enumerate((me, twin)):
        parts = extra[i]
        crest = jnp.max(parts, axis=0, keepdims=True)
        near[slot, pl.ds(home, 1), :] = crest + jnp.log(
            jnp.sum(jnp.exp(parts - crest), axis=0, keepdims=True)
        )
    def tell(i, carry):
        s = (slot + i) % (L * C)
        pltpu.make_async_remote_copy(
            src_ref=near.at[slot], dst_ref=near.at[slot],
            send_sem=near_send, recv_sem=near_recv,
            device_id={"pts": hi * L + s // C, "cen": s % C}, device_id_type=MESH,
        ).start()
        return carry

    lax.fori_loop(1, L * C, tell, 0)
    piece_on(Q * (far - 1))
    for k in (1, 2):
        arrived(far - 1, k, tile_of(far - 1, k))
    second, third, fourth = (tile_of(far - 1, k) for k in (1, 2, 3))
    advance(before, (A, second, False), (A, third, False))
    end = from_side(0, far)
    arrived(far - 1, 3, fourth)
    advance(third, (A, fourth, False), (A, end, False))

    near_group = near.at[pl.ds(0, L * C - 1)]
    pltpu.make_async_copy(near_group, near_group, near_recv).wait()

    def merge(logs):
        crest = jnp.max(logs, axis=0)
        return crest + jnp.log(jnp.sum(jnp.exp(logs - crest[None]), axis=0))

    wide[hi] = merge(near[...])

    def spread(i, carry):
        h = (hi + i) % H
        pltpu.make_async_remote_copy(
            src_ref=wide.at[hi], dst_ref=wide.at[hi],
            send_sem=wide_send, recv_sem=wide_recv,
            device_id={"pts": h * L + me % L, "cen": cen}, device_id_type=MESH,
        ).start()
        return carry

    lax.fori_loop(1, H, spread, 0)
    for i in range(Q // 2):
        twin_copy(0, far, i, end + other).wait_recv()
        twin_copy(1, far, Q - 1 - i, end + other).wait_recv()
    advance(end, (A, end + other, False))
    peak = jnp.max(tops[...], axis=0, keepdims=True)
    for r in range(NS):
        weigh(end + other, r, peak, jnp.zeros((8, T), jnp.float32))
    peaks[pl.ds(end + other, 1), :] = peak * (2.0 * inv_temp)

    wide_group = wide.at[pl.ds(0, H - 1)]
    pltpu.make_async_copy(wide_group, wide_group, wide_recv).wait()
    log_norm = merge(wide[...])
    factors[...] = log_norm
    norm_ref[...] = factors[pl.ds(me, 1), :]
    factors[...] = jnp.exp(peaks[...] - log_norm)

    def scale(j, carry):
        columns = factors[pl.ds(pl.multiple_of(j * 8, 8), 8), :].T
        for i in range(8):
            rows = pl.ds(pl.multiple_of((j * 8 + i) * T, T), T)
            pts_scaled[rows, :] = (
                pts_all[rows, :].astype(jnp.float32) * columns[:, i:i + 1]
            ).astype(jnp.bfloat16)
        return carry

    lax.fori_loop(0, G // 8, scale, 0)

    sent = pts_all.at[pl.ds(0, (G - 1) * T)]
    pltpu.make_async_copy(sent, sent, send_sem).wait()
    pltpu.make_async_copy(near_group, near_group, near_send).wait()
    pltpu.make_async_copy(wide_group, wide_group, wide_send).wait()


def closing(G, shares, pts_scaled, factors, row_ref, tables, out_ref, norm_ref, staged, row, out_sem, row_sem):
    table = tables.at[A]
    own, D = staged.shape
    T = factors.shape[1]
    W = T // 128
    RB = min(256, own)
    NB = own // RB
    row[...] = row_ref[0, :]
    give = pltpu.make_async_copy(row, norm_ref, row_sem)
    give.start()

    KC = min(16, G)

    def update(r, carry):
        rows = pl.ds(pl.multiple_of(r * RB, RB), RB)
        weighted = jnp.zeros((RB, D), jnp.float32)
        mass = jnp.zeros((RB, 128), jnp.float32)
        for j in range(G // KC):
            parts = [shares[j * KC * W + g, rows, :] for g in range(KC * W)]
            weighted += jnp.dot(
                jnp.concatenate(parts, axis=1), pts_scaled[j * KC * T:(j + 1) * KC * T, :],
                preferred_element_type=jnp.float32,
            )
            for g in range(KC * W):
                t, h = j * KC + g // W, g % W
                mass += parts[g].astype(jnp.float32) * factors[t:t + 1, h * 128:(h + 1) * 128]
        total = prior_count + jnp.sum(mass, axis=1, keepdims=True)
        staged[rows, :] = (table[rows, :].astype(jnp.float32) + weighted) / total
        pltpu.make_async_copy(staged.at[rows], out_ref.at[rows], out_sem).start()
        return carry

    lax.fori_loop(0, NB, update, 0, unroll=2 if NB % 2 == 0 else 1)

    give.wait()
    pltpu.make_async_copy(staged, out_ref, out_sem).wait()


def body(G, C, points, centroids):
    T, D = points.shape
    own = centroids.shape[0] // G
    far = G // 4
    L = 1 << ((G.bit_length() - 1) // 2)
    H = G // L
    grant = (66_900_000 - 2 * G * T * (own + D) - 2 * (A + 1) * own * D - 4 * (G + 8) * T) // 1024 * 1024
    vmem, anywhere = pl.BlockSpec(memory_space=pltpu.VMEM), pl.BlockSpec(memory_space=pl.ANY)
    parts = pl.pallas_call(
        functools.partial(kernel, G, C, L),
        out_shape=(
            pltpu.VMEM((G * T // 128, own, 128), jnp.bfloat16),
            pltpu.VMEM((G * T, D), jnp.bfloat16),
            pltpu.VMEM((G, T), jnp.float32),
            pltpu.VMEM((1, T), jnp.float32),
            pltpu.VMEM((A + 1, own, D), jnp.bfloat16),
        ),
        in_specs=[anywhere] * 2,
        out_specs=(vmem,) * 5,
        scratch_shapes=[
            pltpu.VMEM((G * T, D), jnp.bfloat16),
            pltpu.VMEM((own, 128), jnp.float32),
            pltpu.VMEM((own, T), jnp.float32),
            pltpu.VMEM((8, T), jnp.float32),
            pltpu.VMEM((G, T), jnp.float32),
            pltpu.VMEM((2, A + 1, T), jnp.float32),
            pltpu.VMEM((L * C, G, T), jnp.float32),
            pltpu.VMEM((H, G, T), jnp.float32),
            pltpu.SemaphoreType.DMA((A + 2,)),
            pltpu.SemaphoreType.DMA,
            pltpu.SemaphoreType.DMA((2, far + 1, Q)),
            pltpu.SemaphoreType.DMA((2, far + 1, Q)),
            pltpu.SemaphoreType.DMA,
            pltpu.SemaphoreType.DMA,
            pltpu.SemaphoreType.DMA,
            pltpu.SemaphoreType.DMA,
        ],
        compiler_params=pltpu.CompilerParams(
            collective_id=0, has_side_effects=True, vmem_limit_bytes=grant
        ),
    )(points, centroids)
    return pl.pallas_call(
        functools.partial(closing, G),
        out_shape=(
            jax.ShapeDtypeStruct((own, D), jnp.float32),
            jax.ShapeDtypeStruct((T,), jnp.float32),
        ),
        in_specs=[vmem] * 5,
        out_specs=(anywhere, anywhere),
        scratch_shapes=[
            pltpu.VMEM((own, D), jnp.float32),
            pltpu.VMEM((T,), jnp.float32),
            pltpu.SemaphoreType.DMA,
            pltpu.SemaphoreType.DMA,
        ],
        compiler_params=pltpu.CompilerParams(vmem_limit_bytes=16 * 1024 * 1024),
    )(*parts)


def solution(mesh):
    placed = (P("pts", None), P("cen", None))
    return jax.shard_map(
        functools.partial(body, mesh.shape["pts"], mesh.shape["cen"]),
        mesh=mesh,
        in_specs=placed,
        out_specs=(P(("cen", "pts"), None), P("pts")),
        check_vma=False,
    )
```

```python
import functools
import math

import jax
import jax.numpy as jnp
from jax import lax
from jax.experimental import pallas as pl
from jax.experimental.pallas import tpu as pltpu
from jax.sharding import PartitionSpec as P

inv_temp = 0.0625
prior_count = 1.0
log2e = math.log2(math.e)
MESH = pl.DeviceIdType.MESH
Q = 2
A = 3


def kernel(
    G, C, L, points_ref, table_ref, shares, pts_scaled, factors, norm_ref, tables,
    pts_all, half_norms, scores,
    tops, peaks, extra, near, wide,
    load_sem, send_sem, ring_sem, twin_sem, near_send, near_recv, wide_send, wide_recv,
):
    T, D = points_ref.shape
    own = tables.shape[1]
    W = T // 128
    R = G // 2
    far = R // 2
    piece = T // Q
    shift = Q.bit_length() - 1
    H = G // L
    RS = min(1024, own)
    NS = own // RS
    me = lax.axis_index("pts")
    cen = lax.axis_index("cen")
    core = me % 2
    chip = me // 2
    turn = chip % 2
    pos = (chip // 2) * (1 - turn) + (R - 1 - chip // 2) * turn
    other = 1 - 2 * core
    hi = me // L
    slot = (me % L) * C + cen

    def tile_at(p, c):
        return jnp.where(p < far, 2 * p, 2 * (R - 1 - p) + 1) * 2 + c

    twin = me + other
    right = tile_at((pos + 1) % R, core)
    left = tile_at((pos + R - 1) % R, core)

    def around(p):
        return p & (R - 1) if R & (R - 1) == 0 else lax.rem(p, R)

    def from_side(way, d):
        return tile_at(around(pos + R + (2 * way - 1) * d), core)

    my_points = pts_all.at[pl.ds(pl.multiple_of(me * T, T), T)]
    load_points = pltpu.make_async_copy(points_ref, my_points, load_sem.at[0])
    load_points.start()
    blocks = (from_side(0, far - 1), from_side(1, far - 1), from_side(0, far), me)
    loads = [
        pltpu.make_async_copy(
            table_ref.at[pl.ds(pl.multiple_of(block * own, own), own)],
            tables.at[j], load_sem.at[1 + j],
        )
        for j, block in enumerate(blocks)
    ]
    for load in loads:
        load.start()

    barrier = pltpu.get_barrier_semaphore()

    for peer in (right, left, twin):
        pl.semaphore_signal(
            barrier, inc=1, device_id={"pts": peer, "cen": cen}, device_id_type=MESH
        )
    for i in range(1, C):
        for peer in (me, twin):
            pl.semaphore_signal(
                barrier, inc=1, device_id={"pts": peer, "cen": (cen + i) % C}, device_id_type=MESH
            )
    load_points.wait()
    pl.semaphore_wait(barrier, 1 + 2 * C)

    def rows_of(t, q):
        return pts_all.at[pl.ds(pl.multiple_of(t * T + q * piece, piece), piece)]

    def ring_copy(way, d, q, t):
        return pltpu.make_async_remote_copy(
            src_ref=rows_of(t, q), dst_ref=rows_of(t, q), send_sem=send_sem,
            recv_sem=ring_sem.at[way, d, q],
            device_id={"pts": (right, left)[way], "cen": cen}, device_id_type=MESH,
        )

    def twin_copy(way, d, q, t):
        return pltpu.make_async_remote_copy(
            src_ref=rows_of(t, q), dst_ref=rows_of(t, q), send_sem=send_sem,
            recv_sem=twin_sem.at[way, d, q],
            device_id={"pts": twin, "cen": cen}, device_id_type=MESH,
        )

    for i in range(Q):
        ring_copy(0, 1, i, me).start()
        ring_copy(1, 1, Q - 1 - i, me).start()
    for q in range(Q):
        twin_copy(0, 0, q, me).start()

    def pass_on(d, i):
        for way in range(2):
            q = i if way == 0 else Q - 1 - i
            t = from_side(way, d)
            ring_copy(way, d, q, t).wait_recv()

            @pl.when((d + 1 < far) | ((d + 1 == far) & (i < Q // 2)))
            def _():
                ring_copy(way, d + 1, q, t).start()

            twin_copy(way, d, q, t).start()

    near[slot] = jnp.full((G, T), -1e30, jnp.float32)

    lowest = jnp.full((8, T), -jnp.inf, jnp.float32)

    def score(j, tile, r, top, fresh):
        rows = slice(r * RS, (r + 1) * RS)
        block = tables[j, rows, :]
        if fresh:
            wide_block = block.astype(jnp.float32)
            total = jnp.sum(wide_block * wide_block, axis=1, keepdims=True)
            half_norms[rows, :] = jnp.broadcast_to(0.5 * total, (RS, 128))
        u = lax.dot_general(
            block, tile, (((1,), (1,)), ((), ())), preferred_element_type=jnp.float32
        ) - jnp.concatenate([half_norms[rows, :]] * W, axis=1)
        scores[rows, :] = u
        return jnp.maximum(top, jnp.max(u.reshape(RS // 8, 8, T), axis=0))

    def weigh(t, r, peak, total):
        rows = slice(r * RS, (r + 1) * RS)
        e = jnp.exp2((scores[rows, :] - peak) * (2.0 * inv_temp * log2e))
        if t is not None:
            packed = e.astype(jnp.bfloat16)
            for g in range(W):
                shares[t * W + g, rows, :] = packed[:, g * 128:(g + 1) * 128]
        return total + jnp.sum(e.reshape(RS // 8, 8, T), axis=0)

    def finish(t, peak, total):
        scaled = peak * (2.0 * inv_temp)
        if t is not None:
            peaks[pl.ds(t, 1), :] = scaled
        return scaled + jnp.log(jnp.sum(total, axis=0, keepdims=True))

    def points_of(t):
        return pts_all[pl.ds(pl.multiple_of(t * T, T), T), :]

    def advance(before, *then):
        top, values = tops[...], []
        for j, t, fresh in then:
            tile = points_of(t)
            peak = jnp.max(top, axis=0, keepdims=True)
            top, total = lowest, jnp.zeros((8, T), jnp.float32)
            for r in range(NS):
                total = weigh(before, r, peak, total)
                top = score(j, tile, r, top, fresh)
            values.append(finish(before, peak, total))
            before = None if before is None else t
        tops[...] = top
        return values

    def piece_on(m):
        pass_on(1 + (m >> shift), m & (Q - 1))

    loads[0].wait()
    tile = points_of(me)
    top = lowest
    for r in range(NS):
        top = score(0, tile, r, top, True)
    tops[...] = top
    for q in range(Q):
        twin_copy(0, 0, q, twin).wait_recv()

    def borrow(j, carry):
        @pl.when(j > 1)
        def _():
            piece_on(j - 2)

        pltpu.make_async_copy(
            table_ref.at[pl.ds(0, own)], tables.at[j + 1], load_sem.at[j + 2]
        ).wait()
        mine, twins = advance(None, (j, twin, False), (j + 1, me, True))
        extra[0, pl.ds(j, 1), :] = mine
        extra[1, pl.ds(j, 1), :] = twins
        return carry

    lax.fori_loop(0, A, borrow, 0)

    def tile_of(d, k):
        side = k & 1
        t = from_side(0, d) * (1 - side) + from_side(1, d) * side
        return t + jnp.where(k >= 2, other, 0)

    def arrived(d, k, t):
        for way in range(2):
            @pl.when(k == 2 + way)
            def _():
                for q in range(Q):
                    twin_copy(way, d, q, t).wait_recv()

    def step(p, before):
        piece_on(p + A - 2)
        j = 2 * p - 1
        d0, k0, d1, k1 = 1 + (j >> 2), j & 3, 1 + ((j + 1) >> 2), (j + 1) & 3
        t0 = jnp.where(p == 0, twin, tile_of(d0, k0))
        t1 = tile_of(d1, k1)

        @pl.when(p > 0)
        def _():
            arrived(d0, k0, t0)

        arrived(d1, k1, t1)
        first, second = advance(before, (A, t0, False), (A, t1, False))

        @pl.when(p == 0)
        def _():
            extra[0, A:A + 1, :] = first
            extra[1, A:A + 1, :] = second

        @pl.when(p > 0)
        def _():
            near[slot, pl.ds(before, 1), :] = first
            near[slot, pl.ds(t0, 1), :] = second

        return t1

    before = lax.fori_loop(0, 2 * far - 4, step, me)
    t = tile_of(far - 2, 3)
    arrived(far - 2, 3, t)
    near[slot, pl.ds(before, 1), :] = advance(before, (A, t, False))[0]
    peak = jnp.max(tops[...], axis=0, keepdims=True)
    total = jnp.zeros((8, T), jnp.float32)
    for r in range(NS):
        total = weigh(t, r, peak, total)
    near[slot, pl.ds(t, 1), :] = finish(t, peak, total)
    for i, home in enumerate((me, twin)):
        parts = extra[i]
        crest = jnp.max(parts, axis=0, keepdims=True)
        near[slot, pl.ds(home, 1), :] = crest + jnp.log(
            jnp.sum(jnp.exp(parts - crest), axis=0, keepdims=True)
        )
    def tell(i, carry):
        s = (slot + i) % (L * C)
        pltpu.make_async_remote_copy(
            src_ref=near.at[slot], dst_ref=near.at[slot],
            send_sem=near_send, recv_sem=near_recv,
            device_id={"pts": hi * L + s // C, "cen": s % C}, device_id_type=MESH,
        ).start()
        return carry

    lax.fori_loop(1, L * C, tell, 0)
    piece_on(Q * (far - 1) - 1)
    piece_on(Q * (far - 1))
    before = tile_of(far - 1, 0)
    tile = points_of(before)
    top = lowest
    for r in range(NS):
        top = score(A, tile, r, top, False)
    tops[...] = top
    for k in (1, 2):
        arrived(far - 1, k, tile_of(far - 1, k))
    second, third, fourth = (tile_of(far - 1, k) for k in (1, 2, 3))
    advance(before, (A, second, False), (A, third, False))
    end = from_side(0, far)
    arrived(far - 1, 3, fourth)
    advance(third, (A, fourth, False), (A, end, False))

    near_group = near.at[pl.ds(0, L * C - 1)]
    pltpu.make_async_copy(near_group, near_group, near_recv).wait()

    def merge(logs):
        crest = jnp.max(logs, axis=0)
        return crest + jnp.log(jnp.sum(jnp.exp(logs - crest[None]), axis=0))

    wide[hi] = merge(near[...])

    def spread(i, carry):
        h = (hi + i) % H
        pltpu.make_async_remote_copy(
            src_ref=wide.at[hi], dst_ref=wide.at[hi],
            send_sem=wide_send, recv_sem=wide_recv,
            device_id={"pts": h * L + me % L, "cen": cen}, device_id_type=MESH,
        ).start()
        return carry

    lax.fori_loop(1, H, spread, 0)
    for i in range(Q // 2):
        twin_copy(0, far, i, end + other).wait_recv()
        twin_copy(1, far, Q - 1 - i, end + other).wait_recv()
    advance(end, (A, end + other, False))
    peak = jnp.max(tops[...], axis=0, keepdims=True)
    for r in range(NS):
        weigh(end + other, r, peak, jnp.zeros((8, T), jnp.float32))
    peaks[pl.ds(end + other, 1), :] = peak * (2.0 * inv_temp)

    wide_group = wide.at[pl.ds(0, H - 1)]
    pltpu.make_async_copy(wide_group, wide_group, wide_recv).wait()
    log_norm = merge(wide[...])
    factors[...] = log_norm
    norm_ref[...] = factors[pl.ds(me, 1), :]
    factors[...] = jnp.exp(peaks[...] - log_norm)

    def scale(j, carry):
        columns = factors[pl.ds(pl.multiple_of(j * 8, 8), 8), :].T
        for i in range(8):
            rows = pl.ds(pl.multiple_of((j * 8 + i) * T, T), T)
            pts_scaled[rows, :] = (
                pts_all[rows, :].astype(jnp.float32) * columns[:, i:i + 1]
            ).astype(jnp.bfloat16)
        return carry

    lax.fori_loop(0, G // 8, scale, 0, unroll=G <= 16)

    sent = pts_all.at[pl.ds(0, (G - 1) * T)]
    pltpu.make_async_copy(sent, sent, send_sem).wait()
    pltpu.make_async_copy(near_group, near_group, near_send).wait()
    pltpu.make_async_copy(wide_group, wide_group, wide_send).wait()


def closing(G, shares, pts_scaled, factors, row_ref, tables, out_ref, norm_ref, staged, row, out_sem, row_sem):
    table = tables.at[A]
    own, D = staged.shape
    T = factors.shape[1]
    W = T // 128
    RB = min(256, own)
    NB = own // RB
    row[...] = row_ref[0, :]
    give = pltpu.make_async_copy(row, norm_ref, row_sem)
    give.start()

    KC = min(16, G)

    def update(r, carry):
        rows = pl.ds(pl.multiple_of(r * RB, RB), RB)
        weighted = jnp.zeros((RB, D), jnp.float32)
        mass = jnp.zeros((RB, 128), jnp.float32)
        for j in range(G // KC):
            parts = [shares[j * KC * W + g, rows, :] for g in range(KC * W)]
            weighted += jnp.dot(
                jnp.concatenate(parts, axis=1), pts_scaled[j * KC * T:(j + 1) * KC * T, :],
                preferred_element_type=jnp.float32,
            )
            for g in range(KC * W):
                t, h = j * KC + g // W, g % W
                mass += parts[g].astype(jnp.float32) * factors[t:t + 1, h * 128:(h + 1) * 128]
        total = prior_count + jnp.sum(mass, axis=1, keepdims=True)
        staged[rows, :] = (table[rows, :].astype(jnp.float32) + weighted) / total
        pltpu.make_async_copy(staged.at[rows], out_ref.at[rows], out_sem).start()
        return carry

    lax.fori_loop(0, NB, update, 0, unroll=2 if NB % 2 == 0 else 1)

    give.wait()
    pltpu.make_async_copy(staged, out_ref, out_sem).wait()


def body(G, C, points, centroids):
    T, D = points.shape
    own = centroids.shape[0] // G
    far = G // 4
    L = 1 << ((G.bit_length() - 1) // 2)
    H = G // L
    grant = (66_900_000 - 2 * G * T * (own + D) - 2 * (A + 1) * own * D - 4 * (G + 8) * T) // 1024 * 1024
    vmem, anywhere = pl.BlockSpec(memory_space=pltpu.VMEM), pl.BlockSpec(memory_space=pl.ANY)
    parts = pl.pallas_call(
        functools.partial(kernel, G, C, L),
        out_shape=(
            pltpu.VMEM((G * T // 128, own, 128), jnp.bfloat16),
            pltpu.VMEM((G * T, D), jnp.bfloat16),
            pltpu.VMEM((G, T), jnp.float32),
            pltpu.VMEM((1, T), jnp.float32),
            pltpu.VMEM((A + 1, own, D), jnp.bfloat16),
        ),
        in_specs=[anywhere] * 2,
        out_specs=(vmem,) * 5,
        scratch_shapes=[
            pltpu.VMEM((G * T, D), jnp.bfloat16),
            pltpu.VMEM((own, 128), jnp.float32),
            pltpu.VMEM((own, T), jnp.float32),
            pltpu.VMEM((8, T), jnp.float32),
            pltpu.VMEM((G, T), jnp.float32),
            pltpu.VMEM((2, A + 1, T), jnp.float32),
            pltpu.VMEM((L * C, G, T), jnp.float32),
            pltpu.VMEM((H, G, T), jnp.float32),
            pltpu.SemaphoreType.DMA((A + 2,)),
            pltpu.SemaphoreType.DMA,
            pltpu.SemaphoreType.DMA((2, far + 1, Q)),
            pltpu.SemaphoreType.DMA((2, far + 1, Q)),
            pltpu.SemaphoreType.DMA,
            pltpu.SemaphoreType.DMA,
            pltpu.SemaphoreType.DMA,
            pltpu.SemaphoreType.DMA,
        ],
        compiler_params=pltpu.CompilerParams(
            collective_id=0, has_side_effects=True, vmem_limit_bytes=grant
        ),
    )(points, centroids)
    return pl.pallas_call(
        functools.partial(closing, G),
        out_shape=(
            jax.ShapeDtypeStruct((own, D), jnp.float32),
            jax.ShapeDtypeStruct((T,), jnp.float32),
        ),
        in_specs=[vmem] * 5,
        out_specs=(anywhere, anywhere),
        scratch_shapes=[
            pltpu.VMEM((own, D), jnp.float32),
            pltpu.VMEM((T,), jnp.float32),
            pltpu.SemaphoreType.DMA,
            pltpu.SemaphoreType.DMA,
        ],
        compiler_params=pltpu.CompilerParams(vmem_limit_bytes=16 * 1024 * 1024),
    )(*parts)


def solution(mesh):
    placed = (P("pts", None), P("cen", None))
    return jax.shard_map(
        functools.partial(body, mesh.shape["pts"], mesh.shape["cen"]),
        mesh=mesh,
        in_specs=placed,
        out_specs=(P(("cen", "pts"), None), P("pts")),
        check_vma=False,
    )
```
